256 devices in a mesh: row: 8 (over y, core), col: 32 (over x, z).
Axes of the slice: x: 4, y: 4, z: 8, core: 2. Of those that a mesh axis runs over, the one named last changes fastest.
Arguments:
- phases: int32 [8, 32, 8, 24, 576], P('row', 'col'), may hold values from 0 to 2
- grain: float32 [8, 32, 8, 24, 576], P('row', 'col'), may hold values from 0.5 to 2
- phase_cond: float32 [3], replicated, may hold values from 0.3 to 3
- micro_counts: int32 [8, 32, 8], P('row', 'col'), may hold values from 6 to 12, as said below
- current: float32 [8, 32, 8], P('row', 'col'), may hold values from -5 to 5
- load: float32 [8, 32, 8], P('row', 'col'), may hold values from -16 to 16
Outputs:
- states: float32 [8, 32, 8, 3, 24, 576], P('row', 'col')
- tangent: float32 [8, 32, 8, 3, 3], P('row', 'col')
- increment: float32 [8, 32, 8], P('row', 'col')
- residual: float32 [8, 32, 8], P('row', 'col')
The draws below stay inside these ranges and needn't reach their ends.
Inputs may be any that keep to these rules, and one draw needn't show every extreme that they name: `micro_counts`: every draw has an element with 12 inner iterations and one with 6.
All inputs are finite; a program needn't handle non-finite values.
Results may differ from the reference program's by a relative error of at most 0.0003.
Values sent between devices are 32-bit elements; how exact they have to be, the bound alone decides.
A program may use at most 64 MiB of HBM per device.

```python
import math
import jax
import jax.numpy as jnp
from jax import lax

VOX = 24
YZ = 576
PHASES = 3
EZ = 8
MICRO_MAX = 12
MICRO_MIN = 6
MACRO_ITERS = 8
NEX = 8
NEY = 32


def draw_micro_counts(key, part):
    first_key, second_key = jax.random.split(jax.random.fold_in(key, 11))
    base = jax.random.randint(first_key, (NEX, NEY, 1), MICRO_MIN, MICRO_MAX + 1)
    jitter = jax.random.randint(second_key, (NEX, NEY, EZ), -1, 2)
    counts = jnp.clip(base + jitter, MICRO_MIN, MICRO_MAX)
    counts = counts.at[0, 0, 0].set(MICRO_MAX).at[0, 0, 1].set(MICRO_MIN)
    return counts.astype(jnp.int32)


def draw_load(key, part):
    along_x = jnp.arange(NEX, dtype=jnp.float32)[:, None, None] / (NEX - 1)
    along_y = jnp.arange(NEY, dtype=jnp.float32)[None, :, None] / (NEY - 1)
    scale = (1.0 + along_x) * (1.0 + along_y)
    sub_key = jax.random.fold_in(key, 23)
    values = jnp.clip(jax.random.normal(sub_key, (NEX, NEY, EZ), jnp.float32), -4.0, 4.0)
    return (scale * values).astype(jnp.float32)


def plant(entries, own_key, least, high):
    spot = [jax.random.randint(jax.random.fold_in(own_key, axis), (), 0, length) for axis, length in enumerate(entries.shape)]
    longest = entries.shape.index(max(entries.shape))
    next_to = spot[:longest] + [(spot[longest] + 1) % entries.shape[longest]] + spot[longest + 1:]
    return entries.at[tuple(spot)].set(least).at[tuple(next_to)].set(high)


def block_levels(stream_key, extent, shards, least, top_value):
    def one(position, shards_of):
        heights = jax.random.uniform(jax.random.fold_in(jax.random.fold_in(stream_key, 6), position), (shards_of,), jnp.float32, least / len(shards), top_value / len(shards))
        return jnp.repeat(jnp.exp(heights), extent[position] // shards_of).reshape((-1,) + (1,) * (len(extent) - position - 1))

    loudness = one(*shards[0])
    for cut in shards[1:]:
        loudness = loudness * one(*cut)
    return loudness


def noise(rng, shape, deviation, most, cuts=(), kind=jnp.bfloat16):
    gain = block_levels(rng, shape, cuts, -0.22, 0.18) if cuts else 1.0
    entries = jax.random.normal(rng, shape, jnp.float32) * deviation * gain
    return jnp.minimum(jnp.maximum(entries, -most), most).astype(kind)


def setup_inputs(seed: int = 0) -> dict:
    seeds = jax.random.split(jax.random.key(seed), 7)
    phases = plant(jax.random.randint(seeds[0], (NEX, NEY, EZ, VOX, YZ), 0, PHASES), jax.random.fold_in(seeds[0], 1), 0, PHASES - 1).astype(jnp.int32)
    grain = jnp.clip(jnp.exp(math.log(2.0) - 1.3862944 * jax.random.uniform(seeds[1], (NEX, NEY, EZ, VOX, YZ), jnp.float32) ** block_levels(seeds[1], (NEX, NEY, EZ, VOX, YZ), ((0, 8), (1, 32)), -0.2, 0.2)), 0.5, 2.0)
    phase_cond = jnp.clip(jnp.exp(jax.random.uniform(seeds[2], (PHASES,), jnp.float32, math.log(0.3), math.log(3.0))), 0.3, 3.0)
    micro_counts = draw_micro_counts(jax.random.fold_in(seeds[6], 71), 0)
    current = noise(seeds[4], (NEX, NEY, EZ), 1.0, 5.0, ((0, 8), (1, 32)), jnp.float32)
    load = draw_load(jax.random.fold_in(seeds[6], 71), 0)
    return {"phases": phases, "grain": grain, "phase_cond": phase_cond, "micro_counts": micro_counts, "current": current, "load": load}


def forward(field, axis_id):
    z_index = jnp.arange(YZ) % VOX
    if axis_id == 0:
        return jnp.roll(field, -1, axis=-2)
    if axis_id == 1:
        return jnp.roll(field, -VOX, axis=-1)
    return jnp.where(z_index == VOX - 1, jnp.roll(field, VOX - 1, axis=-1), jnp.roll(field, -1, axis=-1))


def behind(field, axis_id):
    z_index = jnp.arange(YZ) % VOX
    if axis_id == 0:
        return jnp.roll(field, 1, axis=-2)
    if axis_id == 1:
        return jnp.roll(field, VOX, axis=-1)
    return jnp.where(z_index == 0, jnp.roll(field, 1 - VOX, axis=-1), jnp.roll(field, 1, axis=-1))


def solve_rve(conduct, count):
    faces = [(conduct + forward(conduct, axis_id)) * 0.5 for axis_id in range(3)]
    back_faces = [behind(faces[axis_id], axis_id) for axis_id in range(3)]
    rhs = jnp.stack([faces[axis_id] - back_faces[axis_id] for axis_id in range(3)])

    def operate(field):
        total = jnp.zeros_like(field)
        for axis_id in range(3):
            total = total + faces[axis_id] * (field - forward(field, axis_id))
            total = total + back_faces[axis_id] * (field - behind(field, axis_id))
        return total

    def sweep(index, carry):
        fluct, remain, direction, norm_now = carry
        image = operate(direction)
        step_size = norm_now / jnp.sum(direction * image, axis=(1, 2))
        fluct = fluct + step_size[:, None, None] * direction
        remain = remain - step_size[:, None, None] * image
        norm_next = jnp.sum(remain * remain, axis=(1, 2))
        direction = remain + (norm_next / norm_now)[:, None, None] * direction
        return fluct, remain, direction, norm_next

    start = (jnp.zeros_like(rhs), rhs, rhs, jnp.sum(rhs * rhs, axis=(1, 2)))
    fluct = lax.fori_loop(0, count, sweep, start)[0]
    identity = jnp.eye(3, dtype=conduct.dtype)
    rows_out = []
    for axis_id in range(3):
        flux = faces[axis_id][None] * (identity[axis_id][:, None, None] + forward(fluct, axis_id) - fluct)
        rows_out.append(jnp.mean(flux, axis=(1, 2)))
    return fluct, jnp.stack(rows_out)


def neighbour(padded, axis_id, offset):
    lead = padded.ndim - 3
    index = [slice(None)] * lead + [slice(1, -1)] * 3
    length = padded.shape[lead + axis_id]
    index[lead + axis_id] = slice(1 + offset, length - 1 + offset)
    return padded[tuple(index)]


def coarse_apply(k_padded, v_padded):
    centre = neighbour(v_padded, 0, 0)
    total = jnp.zeros_like(centre)
    for axis_id in range(3):
        k_centre = neighbour(k_padded[axis_id], 0, 0)
        for offset in (1, -1):
            cond_face = 0.5 * (k_centre + neighbour(k_padded[axis_id], axis_id, offset))
            total = total + cond_face * (centre - neighbour(v_padded, axis_id, offset))
    return total


def reference(phases, grain, phase_cond, micro_counts, current, load):
    conduct = jnp.zeros(grain.shape, grain.dtype)
    for phase_id in range(PHASES):
        conduct = conduct + jnp.where(phases == phase_id, phase_cond[phase_id], 0.0)
    conduct = conduct * grain
    flat = conduct.reshape(-1, VOX, YZ)
    counts = micro_counts.reshape(-1).astype(jnp.int32)
    fluct, tangent = lax.map(lambda pair: solve_rve(pair[0], pair[1]), (flat, counts))
    states = fluct.reshape(NEX, NEY, EZ, 3, VOX, YZ)
    tangent = tangent.reshape(NEX, NEY, EZ, 3, 3)
    diag = jnp.stack([tangent[..., axis_id, axis_id] for axis_id in range(3)])
    k_padded = jnp.pad(diag, ((0, 0), (1, 1), (1, 1), (1, 1)))
    residual = load - coarse_apply(k_padded, jnp.pad(current, 1))
    increment = jnp.zeros_like(residual)
    direction = residual
    norm_now = jnp.sum(residual * residual)
    for iteration in range(MACRO_ITERS):
        image = coarse_apply(k_padded, jnp.pad(direction, 1))
        step_size = norm_now / jnp.sum(direction * image)
        increment = increment + step_size * direction
        residual = residual - step_size * image
        norm_next = jnp.sum(residual * residual)
        direction = residual + (norm_next / norm_now) * direction
        norm_now = norm_next
    return states, tangent, increment, residual
```

```python
import functools

import jax
import jax.numpy as jnp
from jax import lax
from jax.experimental import pallas as pl
from jax.experimental.pallas import tpu as pltpu
from jax.sharding import PartitionSpec as P

VOX = 24
YZ = 576
PHASES = 3
EZ = 8
MICRO_MAX = 12
MACRO_ITERS = 8
NX = 12
PLANE = 9
CELLS = NX * PLANE
ROWS = EZ * VOX
F32 = jnp.float32
BF16 = jnp.bfloat16
MESH = pl.DeviceIdType.MESH


def lane_iota():
    return lax.broadcasted_iota(jnp.int32, (8, 128), 1)


def roll(v, shift):
    return pltpu.roll(v, shift % 128, 1)


class Shifts:
    def __init__(self):
        lane = lane_iota()
        ys = (lane >> 3) & 7
        zs = lane & 7
        self.y_last, self.y_first = ys == 7, ys == 0
        self.z_last, self.z_first = zs == 7, zs == 0
        self.low = lane < 64

    def x_swap(self, v):
        return roll(v, 64)

    def y_up(self, v):
        return jnp.where(self.y_last, roll(v, 56), roll(v, -8))

    def y_down(self, v):
        return jnp.where(self.y_first, roll(v, -56), roll(v, 8))

    def z_up(self, v):
        return jnp.where(self.z_last, roll(v, 7), roll(v, -1))

    def z_down(self, v):
        return jnp.where(self.z_first, roll(v, -7), roll(v, 1))


def pieces(v, count):
    out = []
    for _ in range(count - 1):
        part = v.astype(BF16)
        out.append(part)
        v = v - part.astype(F32)
    out.append(v.astype(BF16))
    return out


def permutation():
    col = lax.broadcasted_iota(jnp.int32, (YZ, YZ), 1)
    row = lax.broadcasted_iota(jnp.int32, (YZ, YZ), 0)
    group = col >> 6
    y_in = (group * 11) >> 5
    z_in = group - 3 * y_in
    source = (((col >> 3) & 7) * 3 + y_in) * VOX + (col & 7) * 3 + z_in
    return jnp.where(row == source, 1.0, 0.0).astype(BF16)


def total(v):
    return jnp.broadcast_to(jnp.sum(v, axis=1, keepdims=True), (8, 128))


def micro_kernel(
    cond_ref, counts_ref, current_ref, load_ref, phases_ref, grain_ref,
    states_ref, tangent_ref, packed_ref,
    perm, stage, face, rhs, fluct, remain, direct, image, edge,
):
    sh = Shifts()
    cells = [(x, y, z) for x in range(NX) for y in range(3) for z in range(3)]

    def at(x, y, z):
        return x * PLANE + y * 3 + z

    perm[...] = permutation()
    phases = phases_ref[...].reshape(ROWS, YZ)
    conduct = jnp.zeros((ROWS, YZ), F32)
    for phase_id in range(PHASES):
        conduct = jnp.where(phases == phase_id, cond_ref[phase_id], conduct)
    conduct = conduct * grain_ref[...].reshape(ROWS, YZ)
    parts = jnp.concatenate(pieces(conduct, 3), axis=0)
    moved = jnp.dot(parts, perm[...], preferred_element_type=F32)
    moved = (moved[2 * ROWS :] + moved[ROWS : 2 * ROWS]) + moved[:ROWS]
    for j in range(4):
        stage[j, 0:ROWS, :] = moved[:, 128 * j : 128 * j + 128]
    stage[4, 0:ROWS, 0:64] = moved[:, 512:576]

    for x in range(NX):
        for j in range(5):
            low = stage[j, pl.ds(x, 8, stride=VOX), :]
            high = stage[j, pl.ds(x + NX, 8, stride=VOX), :]
            image[x * PLANE + 2 * j] = jnp.where(sh.low, low, roll(high, 64))
            if j < 4:
                image[x * PLANE + 2 * j + 1] = jnp.where(sh.low, roll(low, 64), high)

    for x, y, z in cells:
        t = at(x, y, z)
        here = image[t]
        ahead = image[t + PLANE] if x < NX - 1 else sh.x_swap(image[at(0, y, z)])
        face[t] = (here + ahead) * 0.5
        ahead = image[t + 3] if y < 2 else sh.y_up(image[at(x, 0, z)])
        face[CELLS + t] = (here + ahead) * 0.5
        ahead = image[t + 1] if z < 2 else sh.z_up(image[at(x, y, 0)])
        face[2 * CELLS + t] = (here + ahead) * 0.5

    zero = jnp.zeros((8, 128), F32)
    norms = [zero] * 3
    means = [zero] * 3
    for x, y, z in cells:
        t = at(x, y, z)
        back = [
            face[t - PLANE] if x > 0 else sh.x_swap(face[at(NX - 1, y, z)]),
            face[CELLS + t - 3] if y > 0 else sh.y_down(face[CELLS + at(x, 2, z)]),
            face[2 * CELLS + t - 1] if z > 0 else sh.z_down(face[2 * CELLS + at(x, y, 2)]),
        ]
        for c in range(3):
            here = face[c * CELLS + t]
            value = here - back[c]
            rhs[c * CELLS + t] = value
            remain[c * CELLS + t] = value
            direct[c * CELLS + t] = zero
            fluct[c * CELLS + t] = zero
            norms[c] = norms[c] + value * value
            means[c] = means[c] + here

    sub = lax.broadcasted_iota(jnp.int32, (8, 128), 0)
    counts = jnp.zeros((8, 128), jnp.int32)
    for k in range(EZ):
        counts = jnp.where(sub == k, counts_ref[k], counts)

    def sweep(index, carry):
        norm, alpha, beta = carry
        new_alpha, new_norm, new_beta = [], [], []
        for c in range(3):
            base = c * CELLS

            def renew(x):
                plane = {}
                for y in range(3):
                    for z in range(3):
                        t = base + at(x, y, z)
                        old = direct[t]
                        fluct[t] = fluct[t] + alpha[c] * old
                        plane[y, z] = remain[t] + beta[c] * old
                        direct[t] = plane[y, z]
                return plane

            last = renew(NX - 1)
            here = renew(0)
            before = {}
            for y in range(3):
                for z in range(3):
                    flux = face[at(NX - 1, y, z)] * (last[y, z] - sh.x_swap(here[y, z]))
                    edge[c * PLANE + y * 3 + z] = flux
                    before[y, z] = sh.x_swap(flux)
            acc = zero
            for x in range(NX):
                if x < NX - 2:
                    ahead = renew(x + 1)
                elif x == NX - 2:
                    ahead = {(y, z): direct[base + at(x + 1, y, z)] for y in range(3) for z in range(3)}
                flux_x, flux_y, flux_z = {}, {}, {}
                for y in range(3):
                    for z in range(3):
                        t = at(x, y, z)
                        v = here[y, z]
                        if x < NX - 1:
                            flux_x[y, z] = face[t] * (v - ahead[y, z])
                        else:
                            flux_x[y, z] = edge[c * PLANE + y * 3 + z]
                        up = here[y + 1, z] if y < 2 else sh.y_up(here[0, z])
                        flux_y[y, z] = face[CELLS + t] * (v - up)
                        up = here[y, z + 1] if z < 2 else sh.z_up(here[y, 0])
                        flux_z[y, z] = face[2 * CELLS + t] * (v - up)
                for y in range(3):
                    for z in range(3):
                        t = base + at(x, y, z)
                        down_y = flux_y[y - 1, z] if y > 0 else sh.y_down(flux_y[2, z])
                        down_z = flux_z[y, z - 1] if z > 0 else sh.z_down(flux_z[y, 2])
                        out = (flux_x[y, z] - before[y, z]) + ((flux_y[y, z] - down_y) + (flux_z[y, z] - down_z))
                        image[t] = out
                        acc = acc + here[y, z] * out
                before, here = flux_x, ahead
            step = norm[c] / total(acc)
            new_alpha.append(jnp.where(index < counts, step, 0.0))
        for c in range(3):
            base = c * CELLS
            acc = zero
            for t in range(base, base + CELLS):
                value = remain[t] - new_alpha[c] * image[t]
                remain[t] = value
                acc = acc + value * value
            fresh = total(acc)
            new_norm.append(fresh)
            new_beta.append(fresh / norm[c])
        return tuple(new_norm), tuple(new_alpha), tuple(new_beta)

    norm = tuple(total(v) for v in norms)
    norm, alpha, beta = lax.fori_loop(0, MICRO_MAX, sweep, (norm, (zero,) * 3, (zero,) * 3))

    inner = [[zero] * 3 for _ in range(3)]
    for t in range(CELLS):
        for c in range(3):
            value = fluct[c * CELLS + t] + alpha[c] * direct[c * CELLS + t]
            fluct[c * CELLS + t] = value
            for d in range(3):
                inner[d][c] = inner[d][c] + value * rhs[d * CELLS + t]
    scale = 1.0 / (VOX * YZ)
    tangent = [
        [(total(means[d] - inner[d][c]) if d == c else -total(inner[d][c])) * scale for c in range(3)]
        for d in range(3)
    ]
    lane = lane_iota()
    for d in range(3):
        rows = jnp.where(lane == 0, tangent[d][0], jnp.where(lane == 1, tangent[d][1], tangent[d][2]))
        tangent_ref[:, d, :] = rows[:, 0:3]

    slot = lane >> 3
    message = jnp.where(slot == 0, tangent[0][0], jnp.where(slot == 1, tangent[1][1], tangent[2][2]))
    message = jnp.where((sub == (lane & 7)) & (slot < 3), message, 0.0)
    message = jnp.sum(message, axis=0, keepdims=True)
    low = lax.broadcasted_iota(jnp.int32, (1, 128), 1)
    for k in range(EZ):
        message = jnp.where(low == 24 + k, current_ref[k], message)
        message = jnp.where(low == 32 + k, load_ref[k], message)
    packed_ref[...] = message

    for c in range(3):
        for x in range(NX):
            for j in range(5):
                first = fluct[c * CELLS + x * PLANE + 2 * j]
                second = fluct[c * CELLS + x * PLANE + 2 * j + 1] if j < 4 else zero
                stage[j, pl.ds(c * ROWS + x, 8, stride=VOX), :] = jnp.where(sh.low, first, roll(second, 64))
                stage[j, pl.ds(c * ROWS + x + NX, 8, stride=VOX), :] = jnp.where(sh.low, roll(first, 64), second)
    whole = jnp.concatenate([stage[j, 0 : 3 * ROWS, :] for j in range(4)] + [stage[4, 0 : 3 * ROWS, 0:64]], axis=1)
    parts = jnp.concatenate(pieces(whole, 2), axis=0)
    moved = lax.dot_general(parts, perm[...], (((1,), (1,)), ((), ())), preferred_element_type=F32)
    moved = moved[3 * ROWS :] + moved[: 3 * ROWS]
    for c in range(3):
        states_ref[:, c, :, :] = moved[c * ROWS : (c + 1) * ROWS].reshape(EZ, VOX, YZ)


def micro(phases, grain, phase_cond, counts, current, load):
    smem = pl.BlockSpec(memory_space=pltpu.SMEM)
    vmem = pl.BlockSpec(memory_space=pltpu.VMEM)
    field = pltpu.VMEM((3 * CELLS, 8, 128), F32)
    return pl.pallas_call(
        micro_kernel,
        out_shape=(
            jax.ShapeDtypeStruct((EZ, 3, VOX, YZ), F32),
            jax.ShapeDtypeStruct((EZ, 3, 3), F32),
            jax.ShapeDtypeStruct((1, 128), F32),
        ),
        in_specs=[smem, smem, smem, smem, vmem, vmem],
        out_specs=(vmem, vmem, vmem),
        scratch_shapes=[
            pltpu.VMEM((YZ, YZ), BF16),
            pltpu.VMEM((5, 3 * ROWS, 128), F32),
            field, field, field, field, field, field,
            pltpu.VMEM((3 * PLANE, 8, 128), F32),
        ],
        compiler_params=pltpu.CompilerParams(vmem_limit_bytes=60 * 1024 * 1024),
        name="micro",
    )(phase_cond, counts, current, load, phases, grain)


def coarse_kernel(packed_ref, increment_ref, residual_ref, grid, send_a, recv_a, send_b, recv_b):
    rows, cols = 8, 32
    i, j = lax.axis_index("row"), lax.axis_index("col")
    barrier = pltpu.get_barrier_semaphore()

    def greet_col(s, _):
        pl.semaphore_signal(barrier, inc=1, device_id=(i, lax.rem(j + s, cols)), device_id_type=MESH)
        return 0

    def greet_row(s, _):
        pl.semaphore_signal(barrier, inc=1, device_id=(lax.rem(i + s, rows), j), device_id_type=MESH)
        return 0

    lax.fori_loop(1, cols, greet_col, 0)
    lax.fori_loop(1, rows, greet_row, 0)
    pl.semaphore_wait(barrier, cols + rows - 2)

    def along_col(s):
        return pltpu.make_async_remote_copy(
            src_ref=packed_ref,
            dst_ref=grid.at[i, pl.ds(j, 1)],
            send_sem=send_a.at[s],
            recv_sem=recv_a.at[s],
            device_id=(i, lax.rem(j + s, cols)),
            device_id_type=MESH,
        )

    def along_row(s):
        return pltpu.make_async_remote_copy(
            src_ref=grid.at[i],
            dst_ref=grid.at[i],
            send_sem=send_b.at[s],
            recv_sem=recv_b.at[s],
            device_id=(lax.rem(i + s, rows), j),
            device_id_type=MESH,
        )

    def start_col(s, _):
        along_col(s).start()
        return 0

    def wait_col(s, _):
        along_col(s).wait()
        return 0

    def start_row(s, _):
        along_row(s).start()
        return 0

    def wait_row(s, _):
        along_row(s).wait()
        return 0

    lax.fori_loop(1, cols, start_col, 0)
    grid[i, pl.ds(j, 1), :] = packed_ref[...]
    lax.fori_loop(1, cols, wait_col, 0)
    lax.fori_loop(1, rows, start_row, 0)
    lax.fori_loop(1, rows, wait_row, 0)

    lane = lane_iota()
    slot = lane >> 3
    sub = lax.broadcasted_iota(jnp.int32, (8, 128), 0)
    fields = [[jnp.zeros((8, 128), F32)] * 2 for _ in range(5)]
    for col in range(cols):
        at_col = grid[:, col, :]
        half, place = divmod(col, 16)
        for f in range(5):
            spun = roll(at_col, (place - f) * 8)
            fields[f][half] = jnp.where(slot == place, spun, fields[f][half])
    kx, ky, kz, current, load = fields

    def ahead_y(v):
        spun = [roll(part, -8) for part in v]
        return [jnp.where(slot == 15, spun[1], spun[0]), spun[1]]

    def back_y(v):
        spun = [roll(part, 8) for part in v]
        return [spun[0], jnp.where(slot == 0, spun[0], spun[1])]

    def ahead_z(v):
        return [roll(part, -1) for part in v]

    def back_z(v):
        return [roll(part, 1) for part in v]

    def ahead_x(v):
        return [pltpu.roll(part, 7, 0) for part in v]

    def back_x(v):
        return [pltpu.roll(part, 1, 0) for part in v]

    k_in = lane & 7
    never = lane < 0
    outside = [
        ([sub == 7] * 2, [sub == 0] * 2),
        ([never, slot == 15], [slot == 0, never]),
        ([k_in == 7] * 2, [k_in == 0] * 2),
    ]
    moves = [(ahead_x, back_x), (ahead_y, back_y), (ahead_z, back_z)]
    weights = []
    centre = [jnp.zeros((8, 128), F32)] * 2
    for (pair, masks), k in zip(zip(moves, outside), (kx, ky, kz)):
        for move, mask in zip(pair, masks):
            near = move(k)
            cond = [0.5 * (k[h] + jnp.where(mask[h], 0.0, near[h])) for h in range(2)]
            centre = [centre[h] + cond[h] for h in range(2)]
            weights.append((move, [jnp.where(mask[h], 0.0, cond[h]) for h in range(2)]))

    def apply(v):
        out = [centre[h] * v[h] for h in range(2)]
        for move, weight in weights:
            near = move(v)
            out = [out[h] - weight[h] * near[h] for h in range(2)]
        return out

    def dot(a, b):
        both = a[0] * b[0] + a[1] * b[1]
        both = jnp.sum(both, axis=0, keepdims=True)
        return jnp.broadcast_to(jnp.sum(both, axis=1, keepdims=True), (8, 128))

    image = apply(current)
    residual = [load[h] - image[h] for h in range(2)]
    increment = [jnp.zeros((8, 128), F32)] * 2
    direction = residual
    norm = dot(residual, residual)
    for _ in range(MACRO_ITERS):
        image = apply(direction)
        step = norm / dot(direction, image)
        increment = [increment[h] + step * direction[h] for h in range(2)]
        residual = [residual[h] - step * image[h] for h in range(2)]
        fresh = dot(residual, residual)
        ratio = fresh / norm
        direction = [residual[h] + ratio * direction[h] for h in range(2)]
        norm = fresh

    place = lax.rem(j, 16)

    def own(v):
        part = jnp.where(j < 16, v[0], v[1])
        part = jnp.where((sub == i) & (slot == place), part, 0.0)
        part = jnp.broadcast_to(jnp.sum(part, axis=0, keepdims=True), (8, 128))
        spun = pltpu.roll(part, lax.rem(128 - place * 8, 128), 1)
        return spun[0:1, 0:EZ]

    increment_ref[...] = own(increment)
    residual_ref[...] = own(residual)


def coarse(packed):
    vmem = pl.BlockSpec(memory_space=pltpu.VMEM)
    out = jax.ShapeDtypeStruct((1, EZ), F32)
    return pl.pallas_call(
        coarse_kernel,
        out_shape=(out, out),
        in_specs=[vmem],
        out_specs=(vmem, vmem),
        scratch_shapes=[
            pltpu.VMEM((8, 32, 128), F32),
            pltpu.SemaphoreType.DMA((32,)),
            pltpu.SemaphoreType.DMA((32,)),
            pltpu.SemaphoreType.DMA((8,)),
            pltpu.SemaphoreType.DMA((8,)),
        ],
        compiler_params=pltpu.CompilerParams(collective_id=0, has_side_effects=True),
        name="coarse",
    )(packed)


def shards(phases, grain, phase_cond, micro_counts, current, load):
    states, tangent, packed = micro(
        phases.reshape(EZ, VOX, YZ), grain.reshape(EZ, VOX, YZ), phase_cond,
        micro_counts.reshape(EZ), current.reshape(EZ), load.reshape(EZ),
    )
    increment, residual = coarse(packed)
    return (
        states.reshape(1, 1, EZ, 3, VOX, YZ),
        tangent.reshape(1, 1, EZ, 3, 3),
        increment.reshape(1, 1, EZ),
        residual.reshape(1, 1, EZ),
    )


def solution(mesh):
    in_specs = (
        P("row", "col", None, None, None),
        P("row", "col", None, None, None),
        P(),
        P("row", "col", None),
        P("row", "col", None),
        P("row", "col", None),
    )
    out_specs = (
        P("row", "col", None, None, None, None),
        P("row", "col", None, None, None),
        P("row", "col", None),
        P("row", "col", None),
    )
    return jax.shard_map(shards, mesh=mesh, in_specs=in_specs, out_specs=out_specs, check_vma=False)
```

```python
import functools

import jax
import jax.numpy as jnp
from jax import lax
from jax.experimental import pallas as pl
from jax.experimental.pallas import tpu as pltpu
from jax.sharding import PartitionSpec as P

VOX = 24
YZ = 576
PHASES = 3
EZ = 8
MICRO_MAX = 12
MACRO_ITERS = 8
NX = 12
PLANE = 9
CELLS = NX * PLANE
ROWS = EZ * VOX
HALO = 162
CHUNK = 12
F32 = jnp.float32
BF16 = jnp.bfloat16
MESH = pl.DeviceIdType.MESH


def lane_iota():
    return lax.broadcasted_iota(jnp.int32, (8, 128), 1)


def roll(v, shift):
    return pltpu.roll(v, shift % 128, 1)


class Shifts:
    def __init__(self):
        lane = lane_iota()
        ys = (lane >> 3) & 7
        zs = lane & 7
        self.y_up = self.gather(jnp.where(ys == 7, lane - 56, lane + 8))
        self.y_down = self.gather(jnp.where(ys == 0, lane + 56, lane - 8))
        self.z_up = self.gather(jnp.where(zs == 7, lane - 7, lane + 1))
        self.z_down = self.gather(jnp.where(zs == 0, lane + 7, lane - 1))
        self.low = lane < 64

    def gather(self, source):
        return lambda v: jnp.take_along_axis(v, source, axis=1, mode="promise_in_bounds")

    def x_swap(self, v):
        return roll(v, 64)


def pieces(v, count):
    out = []
    for _ in range(count - 1):
        part = v.astype(BF16)
        out.append(part)
        v = v - part.astype(F32)
    out.append(v.astype(BF16))
    return out


def permutation():
    col = lax.broadcasted_iota(jnp.int32, (YZ, YZ), 1)
    row = lax.broadcasted_iota(jnp.int32, (YZ, YZ), 0)
    group = col >> 6
    y_in = (group * 11) >> 5
    z_in = group - 3 * y_in
    source = (((col >> 3) & 7) * 3 + y_in) * VOX + (col & 7) * 3 + z_in
    return jnp.where(row == source, 1.0, 0.0).astype(BF16)


def total(v):
    return jnp.broadcast_to(jnp.sum(v, axis=1, keepdims=True), (8, 128))


def micro_kernel(
    cond_ref, counts_ref, current_ref, load_ref, phases_ref, grain_ref,
    states_ref, tangent_ref, packed_ref,
    perm, stage, face, low_face, rhs, fluct, remain, direct, image, halo,
):
    sh = Shifts()
    cells = [(x, y, z) for x in range(NX) for y in range(3) for z in range(3)]

    def at(x, y, z):
        return x * PLANE + y * 3 + z

    perm[...] = permutation()
    phases = phases_ref[...].reshape(ROWS, YZ)
    conduct = jnp.zeros((ROWS, YZ), F32)
    for phase_id in range(PHASES):
        conduct = jnp.where(phases == phase_id, cond_ref[phase_id], conduct)
    conduct = conduct * grain_ref[...].reshape(ROWS, YZ)
    parts = jnp.concatenate(pieces(conduct, 3), axis=0)
    moved = jnp.dot(parts, perm[...], preferred_element_type=F32)
    moved = (moved[2 * ROWS :] + moved[ROWS : 2 * ROWS]) + moved[:ROWS]
    for j in range(4):
        stage[j, 0:ROWS, :] = moved[:, 128 * j : 128 * j + 128]
    stage[4, 0:ROWS, 0:64] = moved[:, 512:576]

    for x in range(NX):
        for j in range(5):
            low = stage[j, pl.ds(x, 8, stride=VOX), :]
            high = stage[j, pl.ds(x + NX, 8, stride=VOX), :]
            image[x * PLANE + 2 * j] = jnp.where(sh.low, low, roll(high, 64))
            if j < 4:
                image[x * PLANE + 2 * j + 1] = jnp.where(sh.low, roll(low, 64), high)

    for x in range(NX):
        for z in range(3):
            halo[x * 3 + z] = sh.y_up(image[at(x, 0, z)])
    for x in range(NX):
        for y in range(3):
            halo[36 + x * 3 + y] = sh.z_up(image[at(x, y, 0)])
    for k in range(PLANE):
        halo[144 + k] = sh.x_swap(image[k])
    for x, y, z in cells:
        t = at(x, y, z)
        here = image[t]
        ahead = image[t + PLANE] if x < NX - 1 else halo[144 + y * 3 + z]
        face[t] = (here + ahead) * 0.5
        ahead = image[t + 3] if y < 2 else halo[x * 3 + z]
        face[CELLS + t] = (here + ahead) * 0.5
        ahead = image[t + 1] if z < 2 else halo[36 + x * 3 + y]
        face[2 * CELLS + t] = (here + ahead) * 0.5
    for x in range(NX):
        for z in range(3):
            low_face[x * 3 + z] = sh.y_down(face[CELLS + at(x, 2, z)])
    for x in range(NX):
        for y in range(3):
            low_face[36 + x * 3 + y] = sh.z_down(face[2 * CELLS + at(x, y, 2)])
    for k in range(PLANE):
        low_face[72 + k] = sh.x_swap(face[at(NX - 1, 0, 0) + k])

    zero = jnp.zeros((8, 128), F32)
    norms = [zero] * 3
    means = [zero] * 3
    for x, y, z in cells:
        t = at(x, y, z)
        back = [
            face[t - PLANE] if x > 0 else low_face[72 + y * 3 + z],
            face[CELLS + t - 3] if y > 0 else low_face[x * 3 + z],
            face[2 * CELLS + t - 1] if z > 0 else low_face[36 + x * 3 + y],
        ]
        for c in range(3):
            here = face[c * CELLS + t]
            value = here - back[c]
            rhs[c * CELLS + t] = value
            remain[c * CELLS + t] = value
            direct[c * CELLS + t] = zero
            fluct[c * CELLS + t] = zero
            norms[c] = norms[c] + value * value
            means[c] = means[c] + here

    sub = lax.broadcasted_iota(jnp.int32, (8, 128), 0)
    counts = jnp.zeros((8, 128), jnp.int32)
    for k in range(EZ):
        counts = jnp.where(sub == k, counts_ref[k], counts)

    def update(c, alpha, beta):
        base, edge = c * CELLS, c * HALO
        for first in range(0, NX, CHUNK):
            span = range(first, first + CHUNK)
            plane = {}
            for x in span:
                for k in range(PLANE):
                    t = base + x * PLANE + k
                    old = direct[t]
                    fluct[t] = fluct[t] + alpha * old
                    plane[x, k] = remain[t] + beta * old
                    direct[t] = plane[x, k]
                yield
            for x in span:
                for z in range(3):
                    halo[edge + x * 3 + z] = sh.y_up(plane[x, z])
            for x in span:
                for z in range(3):
                    halo[edge + 72 + x * 3 + z] = sh.y_down(plane[x, 6 + z])
            for x in span:
                for y in range(3):
                    halo[edge + 36 + x * 3 + y] = sh.z_up(plane[x, 3 * y])
            for x in span:
                for y in range(3):
                    halo[edge + 108 + x * 3 + y] = sh.z_down(plane[x, 3 * y + 2])
            if first == 0:
                for k in range(PLANE):
                    halo[edge + 144 + k] = sh.x_swap(plane[0, k])
            if first + CHUNK == NX:
                for k in range(PLANE):
                    halo[edge + 153 + k] = sh.x_swap(plane[NX - 1, k])

    def stencil(c, box):
        base, edge = c * CELLS, c * HALO
        acc = zero
        here = [direct[base + k] for k in range(PLANE)]
        before = [low_face[72 + k] * (halo[edge + 153 + k] - here[k]) for k in range(PLANE)]
        for x in range(NX):
            if x < NX - 1:
                ahead = [direct[base + (x + 1) * PLANE + k] for k in range(PLANE)]
            else:
                ahead = [halo[edge + 144 + k] for k in range(PLANE)]
            for y in range(3):
                if y == 0:
                    flux_y = [low_face[x * 3 + z] * (halo[edge + 72 + x * 3 + z] - here[z]) for z in range(3)]
                flux_z = low_face[36 + x * 3 + y] * (halo[edge + 108 + x * 3 + y] - here[3 * y])
                for z in range(3):
                    k = 3 * y + z
                    t = x * PLANE + k
                    v = here[k]
                    next_x = face[t] * (v - ahead[k])
                    up = here[k + 3] if y < 2 else halo[edge + x * 3 + z]
                    next_y = face[CELLS + t] * (v - up)
                    up = here[k + 1] if z < 2 else halo[edge + 36 + x * 3 + y]
                    next_z = face[2 * CELLS + t] * (v - up)
                    out = (next_x - before[k]) + ((next_y - flux_y[z]) + (next_z - flux_z))
                    image[base + t] = out
                    acc = acc + v * out
                    before[k], flux_y[z], flux_z = next_x, next_y, next_z
            here = ahead
            yield
        box.append(acc)

    def descend(c, alpha, box):
        acc = zero
        for x in range(NX):
            for t in range(c * CELLS + x * PLANE, c * CELLS + (x + 1) * PLANE):
                value = remain[t] - alpha * image[t]
                remain[t] = value
                acc = acc + value * value
            yield
        box.append(acc)

    def together(*parts):
        parts = list(parts)
        while parts:
            for part in list(parts):
                if next(part, part) is part:
                    parts.remove(part)

    def sweep(index, carry):
        norm, alpha, beta, last = carry
        live = index < counts
        box = []
        together(stencil(0, box), update(1, alpha[1], beta[1]))
        step_0 = jnp.where(live, norm[0] / total(box[0]), 0.0)
        norm_2 = total(last)
        together(stencil(1, box), update(2, alpha[2], norm_2 / norm[2]))
        step_1 = jnp.where(live, norm[1] / total(box[1]), 0.0)
        together(stencil(2, box), descend(0, step_0, box))
        acc_2, acc_0 = (box[2], box[3])
        step_2 = jnp.where(live, norm_2 / total(acc_2), 0.0)
        norm_0 = total(acc_0)
        together(descend(1, step_1, box))
        norm_1 = total(box[4])
        together(descend(2, step_2, box))
        together(update(0, step_0, norm_0 / norm[0]))
        return (norm_0, norm_1, norm_2), (step_0, step_1, step_2), (zero, norm_1 / norm[1]), box[5]

    norm = tuple(total(v) for v in norms)
    together(update(0, zero, zero))
    first = (norm, (zero,) * 3, (zero, zero), jnp.where(lane_iota() == 0, norm[2], 0.0))
    norm, alpha, _, _ = lax.fori_loop(0, MICRO_MAX, sweep, first)

    inner = [[zero] * 3 for _ in range(3)]
    for t in range(CELLS):
        for c in range(3):
            value = fluct[c * CELLS + t]
            if c > 0:
                value = value + alpha[c] * direct[c * CELLS + t]
                fluct[c * CELLS + t] = value
            for d in range(3):
                inner[d][c] = inner[d][c] + value * rhs[d * CELLS + t]
    scale = 1.0 / (VOX * YZ)
    tangent = [
        [(total(means[d] - inner[d][c]) if d == c else -total(inner[d][c])) * scale for c in range(3)]
        for d in range(3)
    ]
    lane = lane_iota()
    for d in range(3):
        rows = jnp.where(lane == 0, tangent[d][0], jnp.where(lane == 1, tangent[d][1], tangent[d][2]))
        tangent_ref[:, d, :] = rows[:, 0:3]

    slot = lane >> 3
    message = jnp.where(slot == 0, tangent[0][0], jnp.where(slot == 1, tangent[1][1], tangent[2][2]))
    message = jnp.where((sub == (lane & 7)) & (slot < 3), message, 0.0)
    message = jnp.sum(message, axis=0, keepdims=True)
    low = lax.broadcasted_iota(jnp.int32, (1, 128), 1)
    for k in range(EZ):
        message = jnp.where(low == 24 + k, current_ref[k], message)
        message = jnp.where(low == 32 + k, load_ref[k], message)
    packed_ref[...] = message

    for c in range(3):
        for x in range(NX):
            for j in range(5):
                first = fluct[c * CELLS + x * PLANE + 2 * j]
                second = fluct[c * CELLS + x * PLANE + 2 * j + 1] if j < 4 else zero
                stage[j, pl.ds(c * ROWS + x, 8, stride=VOX), :] = jnp.where(sh.low, first, roll(second, 64))
                stage[j, pl.ds(c * ROWS + x + NX, 8, stride=VOX), :] = jnp.where(sh.low, roll(first, 64), second)
    whole = jnp.concatenate([stage[j, 0 : 3 * ROWS, :] for j in range(4)] + [stage[4, 0 : 3 * ROWS, 0:64]], axis=1)
    parts = jnp.concatenate(pieces(whole, 2), axis=0)
    moved = lax.dot_general(parts, perm[...], (((1,), (1,)), ((), ())), preferred_element_type=F32)
    moved = moved[3 * ROWS :] + moved[: 3 * ROWS]
    for c in range(3):
        states_ref[:, c, :, :] = moved[c * ROWS : (c + 1) * ROWS].reshape(EZ, VOX, YZ)


def micro(phases, grain, phase_cond, counts, current, load):
    smem = pl.BlockSpec(memory_space=pltpu.SMEM)
    vmem = pl.BlockSpec(memory_space=pltpu.VMEM)
    field = pltpu.VMEM((3 * CELLS, 8, 128), F32)
    return pl.pallas_call(
        micro_kernel,
        out_shape=(
            jax.ShapeDtypeStruct((EZ, 3, VOX, YZ), F32),
            jax.ShapeDtypeStruct((EZ, 3, 3), F32),
            jax.ShapeDtypeStruct((1, 128), F32),
        ),
        in_specs=[smem, smem, smem, smem, vmem, vmem],
        out_specs=(vmem, vmem, vmem),
        scratch_shapes=[
            pltpu.VMEM((YZ, YZ), BF16),
            pltpu.VMEM((5, 3 * ROWS, 128), F32),
            field,
            pltpu.VMEM((81, 8, 128), F32),
            field, field, field, field, field,
            pltpu.VMEM((3 * HALO, 8, 128), F32),
        ],
        compiler_params=pltpu.CompilerParams(vmem_limit_bytes=60 * 1024 * 1024),
        name="micro",
    )(phase_cond, counts, current, load, phases, grain)


def coarse_kernel(packed_ref, increment_ref, residual_ref, grid, send_a, recv_a, send_b, recv_b):
    rows, cols = 8, 32
    i, j = lax.axis_index("row"), lax.axis_index("col")
    barrier = pltpu.get_barrier_semaphore()

    def greet_col(s, _):
        pl.semaphore_signal(barrier, inc=1, device_id=(i, lax.rem(j + s, cols)), device_id_type=MESH)
        return 0

    def greet_row(s, _):
        pl.semaphore_signal(barrier, inc=1, device_id=(lax.rem(i + s, rows), j), device_id_type=MESH)
        return 0

    lax.fori_loop(1, cols, greet_col, 0)
    lax.fori_loop(1, rows, greet_row, 0)
    pl.semaphore_wait(barrier, cols + rows - 2)

    def along_col(s):
        return pltpu.make_async_remote_copy(
            src_ref=packed_ref,
            dst_ref=grid.at[i, pl.ds(j, 1)],
            send_sem=send_a.at[s],
            recv_sem=recv_a.at[s],
            device_id=(i, lax.rem(j + s, cols)),
            device_id_type=MESH,
        )

    def along_row(s):
        return pltpu.make_async_remote_copy(
            src_ref=grid.at[i],
            dst_ref=grid.at[i],
            send_sem=send_b.at[s],
            recv_sem=recv_b.at[s],
            device_id=(lax.rem(i + s, rows), j),
            device_id_type=MESH,
        )

    def start_col(s, _):
        along_col(s).start()
        return 0

    def wait_col(s, _):
        along_col(s).wait()
        return 0

    def start_row(s, _):
        along_row(s).start()
        return 0

    def wait_row(s, _):
        along_row(s).wait()
        return 0

    lax.fori_loop(1, cols, start_col, 0)
    grid[i, pl.ds(j, 1), :] = packed_ref[...]
    lax.fori_loop(1, cols, wait_col, 0)
    lax.fori_loop(1, rows, start_row, 0)
    lax.fori_loop(1, rows, wait_row, 0)

    lane = lane_iota()
    slot = lane >> 3
    sub = lax.broadcasted_iota(jnp.int32, (8, 128), 0)
    fields = [[jnp.zeros((8, 128), F32)] * 2 for _ in range(5)]
    for col in range(cols):
        at_col = grid[:, col, :]
        half, place = divmod(col, 16)
        for f in range(5):
            spun = roll(at_col, (place - f) * 8)
            fields[f][half] = jnp.where(slot == place, spun, fields[f][half])
    kx, ky, kz, current, load = fields

    def ahead_y(v):
        spun = [roll(part, -8) for part in v]
        return [jnp.where(slot == 15, spun[1], spun[0]), spun[1]]

    def back_y(v):
        spun = [roll(part, 8) for part in v]
        return [spun[0], jnp.where(slot == 0, spun[0], spun[1])]

    def ahead_z(v):
        return [roll(part, -1) for part in v]

    def back_z(v):
        return [roll(part, 1) for part in v]

    def ahead_x(v):
        return [pltpu.roll(part, 7, 0) for part in v]

    def back_x(v):
        return [pltpu.roll(part, 1, 0) for part in v]

    k_in = lane & 7
    never = lane < 0
    outside = [
        ([sub == 7] * 2, [sub == 0] * 2),
        ([never, slot == 15], [slot == 0, never]),
        ([k_in == 7] * 2, [k_in == 0] * 2),
    ]
    moves = [(ahead_x, back_x), (ahead_y, back_y), (ahead_z, back_z)]
    weights = []
    centre = [jnp.zeros((8, 128), F32)] * 2
    for (pair, masks), k in zip(zip(moves, outside), (kx, ky, kz)):
        for move, mask in zip(pair, masks):
            near = move(k)
            cond = [0.5 * (k[h] + jnp.where(mask[h], 0.0, near[h])) for h in range(2)]
            centre = [centre[h] + cond[h] for h in range(2)]
            weights.append((move, [jnp.where(mask[h], 0.0, cond[h]) for h in range(2)]))

    def apply(v):
        out = [centre[h] * v[h] for h in range(2)]
        for move, weight in weights:
            near = move(v)
            out = [out[h] - weight[h] * near[h] for h in range(2)]
        return out

    def dot(a, b):
        both = a[0] * b[0] + a[1] * b[1]
        both = jnp.sum(both, axis=0, keepdims=True)
        return jnp.broadcast_to(jnp.sum(both, axis=1, keepdims=True), (8, 128))

    image = apply(current)
    residual = [load[h] - image[h] for h in range(2)]
    increment = [jnp.zeros((8, 128), F32)] * 2
    direction = residual
    norm = dot(residual, residual)
    for _ in range(MACRO_ITERS):
        image = apply(direction)
        step = norm / dot(direction, image)
        increment = [increment[h] + step * direction[h] for h in range(2)]
        residual = [residual[h] - step * image[h] for h in range(2)]
        fresh = dot(residual, residual)
        ratio = fresh / norm
        direction = [residual[h] + ratio * direction[h] for h in range(2)]
        norm = fresh

    place = lax.rem(j, 16)

    def own(v):
        part = jnp.where(j < 16, v[0], v[1])
        part = jnp.where((sub == i) & (slot == place), part, 0.0)
        part = jnp.broadcast_to(jnp.sum(part, axis=0, keepdims=True), (8, 128))
        spun = pltpu.roll(part, lax.rem(128 - place * 8, 128), 1)
        return spun[0:1, 0:EZ]

    increment_ref[...] = own(increment)
    residual_ref[...] = own(residual)


def coarse(packed):
    vmem = pl.BlockSpec(memory_space=pltpu.VMEM)
    out = jax.ShapeDtypeStruct((1, EZ), F32)
    return pl.pallas_call(
        coarse_kernel,
        out_shape=(out, out),
        in_specs=[vmem],
        out_specs=(vmem, vmem),
        scratch_shapes=[
            pltpu.VMEM((8, 32, 128), F32),
            pltpu.SemaphoreType.DMA((32,)),
            pltpu.SemaphoreType.DMA((32,)),
            pltpu.SemaphoreType.DMA((8,)),
            pltpu.SemaphoreType.DMA((8,)),
        ],
        compiler_params=pltpu.CompilerParams(collective_id=0, has_side_effects=True),
        name="coarse",
    )(packed)


def shards(phases, grain, phase_cond, micro_counts, current, load):
    states, tangent, packed = micro(
        phases.reshape(EZ, VOX, YZ), grain.reshape(EZ, VOX, YZ), phase_cond,
        micro_counts.reshape(EZ), current.reshape(EZ), load.reshape(EZ),
    )
    increment, residual = coarse(packed)
    return (
        states.reshape(1, 1, EZ, 3, VOX, YZ),
        tangent.reshape(1, 1, EZ, 3, 3),
        increment.reshape(1, 1, EZ),
        residual.reshape(1, 1, EZ),
    )


def solution(mesh):
    in_specs = (
        P("row", "col", None, None, None),
        P("row", "col", None, None, None),
        P(),
        P("row", "col", None),
        P("row", "col", None),
        P("row", "col", None),
    )
    out_specs = (
        P("row", "col", None, None, None, None),
        P("row", "col", None, None, None),
        P("row", "col", None),
        P("row", "col", None),
    )
    return jax.shard_map(shards, mesh=mesh, in_specs=in_specs, out_specs=out_specs, check_vma=False)
```

```python
import functools

import jax
import jax.numpy as jnp
from jax import lax
from jax.experimental import pallas as pl
from jax.experimental.pallas import tpu as pltpu
from jax.sharding import PartitionSpec as P

VOX = 24
YZ = 576
PHASES = 3
EZ = 8
MICRO_MAX = 12
MACRO_ITERS = 8
NX = 12
PLANE = 9
CELLS = NX * PLANE
ROWS = EZ * VOX
HALO = 162
CHUNK = 12
F32 = jnp.float32
BF16 = jnp.bfloat16
MESH = pl.DeviceIdType.MESH


def lane_iota():
    return lax.broadcasted_iota(jnp.int32, (8, 128), 1)


def roll(v, shift):
    return pltpu.roll(v, shift % 128, 1)


class Shifts:
    def __init__(self):
        lane = lane_iota()
        ys = (lane >> 3) & 7
        zs = lane & 7
        self.y_up = self.gather(jnp.where(ys == 7, lane - 56, lane + 8))
        self.y_down = self.gather(jnp.where(ys == 0, lane + 56, lane - 8))
        self.z_up = self.gather(jnp.where(zs == 7, lane - 7, lane + 1))
        self.z_down = self.gather(jnp.where(zs == 0, lane + 7, lane - 1))
        self.low = lane < 64

    def gather(self, source):
        return lambda v: jnp.take_along_axis(v, source, axis=1, mode="promise_in_bounds")

    def x_swap(self, v):
        return roll(v, 64)


def pieces(v, count):
    out = []
    for _ in range(count - 1):
        part = v.astype(BF16)
        out.append(part)
        v = v - part.astype(F32)
    out.append(v.astype(BF16))
    return out


def permutation():
    col = lax.broadcasted_iota(jnp.int32, (YZ, YZ), 1)
    row = lax.broadcasted_iota(jnp.int32, (YZ, YZ), 0)
    group = col >> 6
    y_in = (group * 11) >> 5
    z_in = group - 3 * y_in
    source = (((col >> 3) & 7) * 3 + y_in) * VOX + (col & 7) * 3 + z_in
    return jnp.where(row == source, 1.0, 0.0).astype(BF16)


def total(v):
    return jnp.broadcast_to(jnp.sum(v, axis=1, keepdims=True), (8, 128))


def heavy_kernel(
    cond_ref, counts_ref, current_ref, load_ref, phases_ref, grain_ref,
    states_ref, tangent_ref, grid_ref,
    perm, stage, face, low_face, rhs, fluct, remain, direct, image, halo, packed, states,
    send_a, recv_a, send_b, recv_b, out_sem,
):
    rows, cols = 8, 32
    row_at, col_at = lax.axis_index("row"), lax.axis_index("col")
    barrier = pltpu.get_barrier_semaphore()

    def greet_col(s, _):
        pl.semaphore_signal(barrier, inc=1, device_id=(row_at, lax.rem(col_at + s, cols)), device_id_type=MESH)
        return 0

    def greet_row(s, _):
        pl.semaphore_signal(barrier, inc=1, device_id=(lax.rem(row_at + s, rows), col_at), device_id_type=MESH)
        return 0

    lax.fori_loop(1, cols, greet_col, 0)
    lax.fori_loop(1, rows, greet_row, 0)

    sh = Shifts()
    cells = [(x, y, z) for x in range(NX) for y in range(3) for z in range(3)]

    def at(x, y, z):
        return x * PLANE + y * 3 + z

    perm[...] = permutation()
    phases = phases_ref[...].reshape(ROWS, YZ)
    conduct = jnp.zeros((ROWS, YZ), F32)
    for phase_id in range(PHASES):
        conduct = jnp.where(phases == phase_id, cond_ref[phase_id], conduct)
    conduct = conduct * grain_ref[...].reshape(ROWS, YZ)
    parts = jnp.concatenate(pieces(conduct, 3), axis=0)
    moved = jnp.dot(parts, perm[...], preferred_element_type=F32)
    moved = (moved[2 * ROWS :] + moved[ROWS : 2 * ROWS]) + moved[:ROWS]
    for j in range(4):
        stage[j, 0:ROWS, :] = moved[:, 128 * j : 128 * j + 128]
    stage[4, 0:ROWS, 0:64] = moved[:, 512:576]

    for x in range(NX):
        for j in range(5):
            low = stage[j, pl.ds(x, 8, stride=VOX), :]
            high = stage[j, pl.ds(x + NX, 8, stride=VOX), :]
            image[x * PLANE + 2 * j] = jnp.where(sh.low, low, roll(high, 64))
            if j < 4:
                image[x * PLANE + 2 * j + 1] = jnp.where(sh.low, roll(low, 64), high)

    for x in range(NX):
        for z in range(3):
            halo[x * 3 + z] = sh.y_up(image[at(x, 0, z)])
    for x in range(NX):
        for y in range(3):
            halo[36 + x * 3 + y] = sh.z_up(image[at(x, y, 0)])
    for k in range(PLANE):
        halo[144 + k] = sh.x_swap(image[k])
    for x, y, z in cells:
        t = at(x, y, z)
        here = image[t]
        ahead = image[t + PLANE] if x < NX - 1 else halo[144 + y * 3 + z]
        face[t] = (here + ahead) * 0.5
        ahead = image[t + 3] if y < 2 else halo[x * 3 + z]
        face[CELLS + t] = (here + ahead) * 0.5
        ahead = image[t + 1] if z < 2 else halo[36 + x * 3 + y]
        face[2 * CELLS + t] = (here + ahead) * 0.5
    for x in range(NX):
        for z in range(3):
            low_face[x * 3 + z] = sh.y_down(face[CELLS + at(x, 2, z)])
    for x in range(NX):
        for y in range(3):
            low_face[36 + x * 3 + y] = sh.z_down(face[2 * CELLS + at(x, y, 2)])
    for k in range(PLANE):
        low_face[72 + k] = sh.x_swap(face[at(NX - 1, 0, 0) + k])

    zero = jnp.zeros((8, 128), F32)
    norms = [zero] * 3
    means = [zero] * 3
    for x, y, z in cells:
        t = at(x, y, z)
        back = [
            face[t - PLANE] if x > 0 else low_face[72 + y * 3 + z],
            face[CELLS + t - 3] if y > 0 else low_face[x * 3 + z],
            face[2 * CELLS + t - 1] if z > 0 else low_face[36 + x * 3 + y],
        ]
        for c in range(3):
            here = face[c * CELLS + t]
            value = here - back[c]
            rhs[c * CELLS + t] = value
            remain[c * CELLS + t] = value
            direct[c * CELLS + t] = zero
            fluct[c * CELLS + t] = zero
            norms[c] = norms[c] + value * value
            means[c] = means[c] + here

    sub = lax.broadcasted_iota(jnp.int32, (8, 128), 0)
    counts = jnp.zeros((8, 128), jnp.int32)
    for k in range(EZ):
        counts = jnp.where(sub == k, counts_ref[k], counts)

    def update(c, alpha, beta):
        base, edge = c * CELLS, c * HALO
        for first in range(0, NX, CHUNK):
            span = range(first, first + CHUNK)
            plane = {}
            for x in span:
                for k in range(PLANE):
                    t = base + x * PLANE + k
                    old = direct[t]
                    fluct[t] = fluct[t] + alpha * old
                    plane[x, k] = remain[t] + beta * old
                    direct[t] = plane[x, k]
                yield
            for x in span:
                for z in range(3):
                    halo[edge + x * 3 + z] = sh.y_up(plane[x, z])
            for x in span:
                for z in range(3):
                    halo[edge + 72 + x * 3 + z] = sh.y_down(plane[x, 6 + z])
            for x in span:
                for y in range(3):
                    halo[edge + 36 + x * 3 + y] = sh.z_up(plane[x, 3 * y])
            for x in span:
                for y in range(3):
                    halo[edge + 108 + x * 3 + y] = sh.z_down(plane[x, 3 * y + 2])
            if first == 0:
                for k in range(PLANE):
                    halo[edge + 144 + k] = sh.x_swap(plane[0, k])
            if first + CHUNK == NX:
                for k in range(PLANE):
                    halo[edge + 153 + k] = sh.x_swap(plane[NX - 1, k])

    def stencil(c, box):
        base, edge = c * CELLS, c * HALO
        acc = zero
        here = [direct[base + k] for k in range(PLANE)]
        before = [low_face[72 + k] * (halo[edge + 153 + k] - here[k]) for k in range(PLANE)]
        for x in range(NX):
            if x < NX - 1:
                ahead = [direct[base + (x + 1) * PLANE + k] for k in range(PLANE)]
            else:
                ahead = [halo[edge + 144 + k] for k in range(PLANE)]
            for y in range(3):
                if y == 0:
                    flux_y = [low_face[x * 3 + z] * (halo[edge + 72 + x * 3 + z] - here[z]) for z in range(3)]
                flux_z = low_face[36 + x * 3 + y] * (halo[edge + 108 + x * 3 + y] - here[3 * y])
                for z in range(3):
                    k = 3 * y + z
                    t = x * PLANE + k
                    v = here[k]
                    next_x = face[t] * (v - ahead[k])
                    up = here[k + 3] if y < 2 else halo[edge + x * 3 + z]
                    next_y = face[CELLS + t] * (v - up)
                    up = here[k + 1] if z < 2 else halo[edge + 36 + x * 3 + y]
                    next_z = face[2 * CELLS + t] * (v - up)
                    out = (next_x - before[k]) + ((next_y - flux_y[z]) + (next_z - flux_z))
                    image[base + t] = out
                    acc = acc + v * out
                    before[k], flux_y[z], flux_z = next_x, next_y, next_z
            here = ahead
            yield
        box.append(acc)

    def descend(c, alpha, box):
        acc = zero
        for x in range(NX):
            for t in range(c * CELLS + x * PLANE, c * CELLS + (x + 1) * PLANE):
                value = remain[t] - alpha * image[t]
                remain[t] = value
                acc = acc + value * value
            yield
        box.append(acc)

    def together(*parts):
        parts = list(parts)
        while parts:
            for part in list(parts):
                if next(part, part) is part:
                    parts.remove(part)

    def sweep(index, carry):
        norm, alpha, beta, last = carry
        live = index < counts
        box = []
        together(stencil(0, box), update(1, alpha[1], beta[1]))
        step_0 = jnp.where(live, norm[0] / total(box[0]), 0.0)
        norm_2 = total(last)
        together(stencil(1, box), update(2, alpha[2], norm_2 / norm[2]))
        step_1 = jnp.where(live, norm[1] / total(box[1]), 0.0)
        together(stencil(2, box), descend(0, step_0, box))
        acc_2, acc_0 = (box[2], box[3])
        step_2 = jnp.where(live, norm_2 / total(acc_2), 0.0)
        norm_0 = total(acc_0)
        together(descend(1, step_1, box))
        norm_1 = total(box[4])
        together(descend(2, step_2, box))
        together(update(0, step_0, norm_0 / norm[0]))
        return (norm_0, norm_1, norm_2), (step_0, step_1, step_2), (zero, norm_1 / norm[1]), box[5]

    norm = tuple(total(v) for v in norms)
    together(update(0, zero, zero))
    first = (norm, (zero,) * 3, (zero, zero), jnp.where(lane_iota() == 0, norm[2], 0.0))
    norm, alpha, _, _ = lax.fori_loop(0, MICRO_MAX, sweep, first)

    inner = [[zero] * 3 for _ in range(3)]
    for t in range(CELLS):
        for c in range(3):
            value = fluct[c * CELLS + t]
            if c > 0:
                value = value + alpha[c] * direct[c * CELLS + t]
                fluct[c * CELLS + t] = value
            for d in range(3):
                inner[d][c] = inner[d][c] + value * rhs[d * CELLS + t]
    scale = 1.0 / (VOX * YZ)
    tangent = [
        [(total(means[d] - inner[d][c]) if d == c else -total(inner[d][c])) * scale for c in range(3)]
        for d in range(3)
    ]
    lane = lane_iota()
    for d in range(3):
        for c in range(3):
            spread = jnp.sum(jnp.where(sub == (lane & 7), tangent[d][c], 0.0), axis=0, keepdims=True)
            tangent_ref[d, c] = spread[:, 0:EZ]

    slot = lane >> 3
    message = jnp.where(slot == 0, tangent[0][0], jnp.where(slot == 1, tangent[1][1], tangent[2][2]))
    message = jnp.where((sub == (lane & 7)) & (slot < 3), message, 0.0)
    message = jnp.sum(message, axis=0, keepdims=True)
    low = lax.broadcasted_iota(jnp.int32, (1, 128), 1)
    for k in range(EZ):
        message = jnp.where(low == 24 + k, current_ref[k], message)
        message = jnp.where(low == 32 + k, load_ref[k], message)
    packed[...] = message
    pl.semaphore_wait(barrier, cols + rows - 2)

    def along_col(s):
        return pltpu.make_async_remote_copy(
            src_ref=packed,
            dst_ref=grid_ref.at[row_at, pl.ds(col_at, 1)],
            send_sem=send_a.at[s],
            recv_sem=recv_a.at[s],
            device_id=(row_at, lax.rem(col_at + s, cols)),
            device_id_type=MESH,
        )

    def along_row(s):
        return pltpu.make_async_remote_copy(
            src_ref=grid_ref.at[row_at],
            dst_ref=grid_ref.at[row_at],
            send_sem=send_b.at[s],
            recv_sem=recv_b.at[s],
            device_id=(lax.rem(row_at + s, rows), col_at),
            device_id_type=MESH,
        )

    def start_col(s, _):
        along_col(s).start()
        return 0

    def wait_col(s, _):
        along_col(s).wait()
        return 0

    def start_row(s, _):
        along_row(s).start()
        return 0

    def wait_row(s, _):
        along_row(s).wait()
        return 0

    lax.fori_loop(1, cols, start_col, 0)
    grid_ref[row_at, pl.ds(col_at, 1), :] = message

    for c in range(3):
        for x in range(NX):
            for j in range(5):
                first = fluct[c * CELLS + x * PLANE + 2 * j]
                second = fluct[c * CELLS + x * PLANE + 2 * j + 1] if j < 4 else zero
                stage[j, pl.ds(c * ROWS + x, 8, stride=VOX), :] = jnp.where(sh.low, first, roll(second, 64))
                stage[j, pl.ds(c * ROWS + x + NX, 8, stride=VOX), :] = jnp.where(sh.low, roll(first, 64), second)
    whole = jnp.concatenate([stage[j, 0 : 3 * ROWS, :] for j in range(4)] + [stage[4, 0 : 3 * ROWS, 0:64]], axis=1)
    parts = jnp.concatenate(pieces(whole, 2), axis=0)
    moved = lax.dot_general(parts, perm[...], (((1,), (1,)), ((), ())), preferred_element_type=F32)
    moved = moved[3 * ROWS :] + moved[: 3 * ROWS]
    for c in range(3):
        states[:, c, :, :] = moved[c * ROWS : (c + 1) * ROWS].reshape(EZ, VOX, YZ)
    out = pltpu.make_async_copy(states, states_ref, out_sem)
    out.start()
    lax.fori_loop(1, cols, wait_col, 0)
    lax.fori_loop(1, rows, start_row, 0)
    lax.fori_loop(1, rows, wait_row, 0)
    out.wait()


def heavy(phases, grain, phase_cond, counts, current, load):
    smem = pl.BlockSpec(memory_space=pltpu.SMEM)
    vmem = pl.BlockSpec(memory_space=pltpu.VMEM)
    field = pltpu.VMEM((3 * CELLS, 8, 128), F32)
    return pl.pallas_call(
        heavy_kernel,
        out_shape=(
            jax.ShapeDtypeStruct((EZ, 3, VOX, YZ), F32),
            jax.ShapeDtypeStruct((3, 3, 1, EZ), F32),
            jax.ShapeDtypeStruct((8, 32, 128), F32),
        ),
        in_specs=[smem, smem, smem, smem, vmem, vmem],
        out_specs=(pl.BlockSpec(memory_space=pl.ANY), vmem, vmem),
        scratch_shapes=[
            pltpu.VMEM((YZ, YZ), BF16),
            pltpu.VMEM((5, 3 * ROWS, 128), F32),
            field,
            pltpu.VMEM((81, 8, 128), F32),
            field, field, field, field, field,
            pltpu.VMEM((3 * HALO, 8, 128), F32),
            pltpu.VMEM((1, 128), F32),
            pltpu.VMEM((EZ, 3, VOX, YZ), F32),
            pltpu.SemaphoreType.DMA((32,)),
            pltpu.SemaphoreType.DMA((32,)),
            pltpu.SemaphoreType.DMA((8,)),
            pltpu.SemaphoreType.DMA((8,)),
            pltpu.SemaphoreType.DMA,
        ],
        compiler_params=pltpu.CompilerParams(
            vmem_limit_bytes=62 * 1024 * 1024, collective_id=0, has_side_effects=True
        ),
        name="micro",
    )(phase_cond, counts, current, load, phases, grain)


def coarse_kernel(
    grid, states_in, tangent_in, states_ref, tangent_ref, increment_ref, residual_ref, states, in_sem, out_sem
):
    cols = 32
    i, j = lax.axis_index("row"), lax.axis_index("col")
    inward = [pltpu.make_async_copy(states_in.at[e], states.at[e], in_sem.at[e]) for e in range(EZ)]
    outward = [pltpu.make_async_copy(states.at[e], states_ref.at[e], out_sem.at[e]) for e in range(EZ)]
    for copy in inward:
        copy.start()
    tangent_ref[...] = tangent_in[...]

    lane = lane_iota()
    slot = lane >> 3
    sub = lax.broadcasted_iota(jnp.int32, (8, 128), 0)
    fields = [[jnp.zeros((8, 128), F32)] * 2 for _ in range(5)]
    for col in range(cols):
        at_col = grid[:, col, :]
        half, place = divmod(col, 16)
        for f in range(5):
            spun = roll(at_col, (place - f) * 8)
            fields[f][half] = jnp.where(slot == place, spun, fields[f][half])
    kx, ky, kz, current, load = fields
    for before, after in zip(inward, outward):
        before.wait()
        after.start()

    def ahead_y(v):
        spun = [roll(part, -8) for part in v]
        return [jnp.where(slot == 15, spun[1], spun[0]), spun[1]]

    def back_y(v):
        spun = [roll(part, 8) for part in v]
        return [spun[0], jnp.where(slot == 0, spun[0], spun[1])]

    def ahead_z(v):
        return [roll(part, -1) for part in v]

    def back_z(v):
        return [roll(part, 1) for part in v]

    def ahead_x(v):
        return [pltpu.roll(part, 7, 0) for part in v]

    def back_x(v):
        return [pltpu.roll(part, 1, 0) for part in v]

    k_in = lane & 7
    never = lane < 0
    outside = [
        ([sub == 7] * 2, [sub == 0] * 2),
        ([never, slot == 15], [slot == 0, never]),
        ([k_in == 7] * 2, [k_in == 0] * 2),
    ]
    moves = [(ahead_x, back_x), (ahead_y, back_y), (ahead_z, back_z)]
    weights = []
    centre = [jnp.zeros((8, 128), F32)] * 2
    for (pair, masks), k in zip(zip(moves, outside), (kx, ky, kz)):
        for move, mask in zip(pair, masks):
            near = move(k)
            cond = [0.5 * (k[h] + jnp.where(mask[h], 0.0, near[h])) for h in range(2)]
            centre = [centre[h] + cond[h] for h in range(2)]
            weights.append((move, [jnp.where(mask[h], 0.0, cond[h]) for h in range(2)]))

    def apply(v):
        out = [centre[h] * v[h] for h in range(2)]
        for move, weight in weights:
            near = move(v)
            out = [out[h] - weight[h] * near[h] for h in range(2)]
        return out

    def dot(a, b):
        both = a[0] * b[0] + a[1] * b[1]
        both = jnp.sum(both, axis=0, keepdims=True)
        return jnp.broadcast_to(jnp.sum(both, axis=1, keepdims=True), (8, 128))

    image = apply(current)
    residual = [load[h] - image[h] for h in range(2)]
    increment = [jnp.zeros((8, 128), F32)] * 2
    direction = residual
    norm = dot(residual, residual)
    for _ in range(MACRO_ITERS):
        image = apply(direction)
        step = norm / dot(direction, image)
        increment = [increment[h] + step * direction[h] for h in range(2)]
        residual = [residual[h] - step * image[h] for h in range(2)]
        fresh = dot(residual, residual)
        ratio = fresh / norm
        direction = [residual[h] + ratio * direction[h] for h in range(2)]
        norm = fresh

    place = lax.rem(j, 16)

    def own(v):
        part = jnp.where(j < 16, v[0], v[1])
        part = jnp.where((sub == i) & (slot == place), part, 0.0)
        part = jnp.broadcast_to(jnp.sum(part, axis=0, keepdims=True), (8, 128))
        spun = pltpu.roll(part, lax.rem(128 - place * 8, 128), 1)
        return spun[0:1, 0:EZ]

    increment_ref[...] = own(increment)
    residual_ref[...] = own(residual)
    for copy in outward:
        copy.wait()


def coarse(grid, states, tangent):
    vmem = pl.BlockSpec(memory_space=pltpu.VMEM)
    hbm = pl.BlockSpec(memory_space=pl.ANY)
    out = jax.ShapeDtypeStruct((1, EZ), F32)
    return pl.pallas_call(
        coarse_kernel,
        out_shape=(
            jax.ShapeDtypeStruct((EZ, 3, VOX, YZ), F32),
            jax.ShapeDtypeStruct((3, 3, 1, EZ), F32),
            out,
            out,
        ),
        in_specs=[vmem, hbm, vmem],
        out_specs=(hbm, vmem, vmem, vmem),
        scratch_shapes=[
            pltpu.VMEM((EZ, 3, VOX, YZ), F32),
            pltpu.SemaphoreType.DMA((EZ,)),
            pltpu.SemaphoreType.DMA((EZ,)),
        ],
        name="coarse",
    )(grid, states, tangent)


def shards(phases, grain, phase_cond, micro_counts, current, load):
    states, tangent, grid = heavy(
        phases.reshape(EZ, VOX, YZ), grain.reshape(EZ, VOX, YZ), phase_cond,
        micro_counts.reshape(EZ), current.reshape(EZ), load.reshape(EZ),
    )
    states, tangent, increment, residual = coarse(grid, states, tangent)
    return (
        states.reshape(1, 1, EZ, 3, VOX, YZ),
        jnp.moveaxis(tangent, 3, 0).reshape(1, 1, EZ, 3, 3),
        increment.reshape(1, 1, EZ),
        residual.reshape(1, 1, EZ),
    )


def solution(mesh):
    in_specs = (
        P("row", "col", None, None, None),
        P("row", "col", None, None, None),
        P(),
        P("row", "col", None),
        P("row", "col", None),
        P("row", "col", None),
    )
    out_specs = (
        P("row", "col", None, None, None, None),
        P("row", "col", None, None, None),
        P("row", "col", None),
        P("row", "col", None),
    )
    return jax.shard_map(shards, mesh=mesh, in_specs=in_specs, out_specs=out_specs, check_vma=False)
```

```python
import functools

import jax
import jax.numpy as jnp
from jax import lax
from jax.experimental import pallas as pl
from jax.experimental.pallas import tpu as pltpu
from jax.sharding import PartitionSpec as P

VOX = 24
YZ = 576
PHASES = 3
EZ = 8
MICRO_MAX = 12
MACRO_ITERS = 8
NX = 12
PLANE = 9
CELLS = NX * PLANE
ROWS = EZ * VOX
HALO = 162
CHUNK = 3
F32 = jnp.float32
BF16 = jnp.bfloat16
MESH = pl.DeviceIdType.MESH


def lane_iota():
    return lax.broadcasted_iota(jnp.int32, (8, 128), 1)


def roll(v, shift):
    return pltpu.roll(v, shift % 128, 1)


class Shifts:
    def __init__(self):
        lane = lane_iota()
        ys = (lane >> 3) & 7
        zs = lane & 7
        self.y_up = self.gather(jnp.where(ys == 7, lane - 56, lane + 8))
        self.y_down = self.gather(jnp.where(ys == 0, lane + 56, lane - 8))
        self.z_up = self.gather(jnp.where(zs == 7, lane - 7, lane + 1))
        self.z_down = self.gather(jnp.where(zs == 0, lane + 7, lane - 1))
        self.low = lane < 64

    def gather(self, source):
        return lambda v: jnp.take_along_axis(v, source, axis=1, mode="promise_in_bounds")

    def x_swap(self, v):
        return roll(v, 64)


def pieces(v, count):
    out = []
    for _ in range(count - 1):
        part = v.astype(BF16)
        out.append(part)
        v = v - part.astype(F32)
    out.append(v.astype(BF16))
    return out


def permutation():
    col = lax.broadcasted_iota(jnp.int32, (YZ, YZ), 1)
    row = lax.broadcasted_iota(jnp.int32, (YZ, YZ), 0)
    group = col >> 6
    y_in = (group * 11) >> 5
    z_in = group - 3 * y_in
    source = (((col >> 3) & 7) * 3 + y_in) * VOX + (col & 7) * 3 + z_in
    return jnp.where(row == source, 1.0, 0.0).astype(BF16)


def total(v):
    return jnp.broadcast_to(jnp.sum(v, axis=1, keepdims=True), (8, 128))


def heavy_kernel(
    cond_ref, counts_ref, current_ref, load_ref, phases_ref, grain_ref,
    states_ref, tangent_ref, grid_ref,
    perm, stage, face, low_face, rhs, fluct, remain, direct, image, halo, packed, states,
    send_a, recv_a, send_b, recv_b, out_sem,
):
    rows, cols = 8, 32
    row_at, col_at = lax.axis_index("row"), lax.axis_index("col")
    barrier = pltpu.get_barrier_semaphore()

    def greet_col(s, _):
        pl.semaphore_signal(barrier, inc=1, device_id=(row_at, lax.rem(col_at + s, cols)), device_id_type=MESH)
        return 0

    def greet_row(s, _):
        pl.semaphore_signal(barrier, inc=1, device_id=(lax.rem(row_at + s, rows), col_at), device_id_type=MESH)
        return 0

    lax.fori_loop(1, cols, greet_col, 0)
    lax.fori_loop(1, rows, greet_row, 0)

    sh = Shifts()
    cells = [(x, y, z) for x in range(NX) for y in range(3) for z in range(3)]

    def at(x, y, z):
        return x * PLANE + y * 3 + z

    perm[...] = permutation()
    phases = phases_ref[...].reshape(ROWS, YZ)
    conduct = jnp.zeros((ROWS, YZ), F32)
    for phase_id in range(PHASES):
        conduct = jnp.where(phases == phase_id, cond_ref[phase_id], conduct)
    conduct = conduct * grain_ref[...].reshape(ROWS, YZ)
    parts = jnp.concatenate(pieces(conduct, 3), axis=0)
    moved = jnp.dot(parts, perm[...], preferred_element_type=F32)
    moved = (moved[2 * ROWS :] + moved[ROWS : 2 * ROWS]) + moved[:ROWS]
    for j in range(4):
        stage[j, 0:ROWS, :] = moved[:, 128 * j : 128 * j + 128]
    stage[4, 0:ROWS, 0:64] = moved[:, 512:576]

    for x in range(NX):
        for j in range(5):
            low = stage[j, pl.ds(x, 8, stride=VOX), :]
            high = stage[j, pl.ds(x + NX, 8, stride=VOX), :]
            image[x * PLANE + 2 * j] = jnp.where(sh.low, low, roll(high, 64))
            if j < 4:
                image[x * PLANE + 2 * j + 1] = jnp.where(sh.low, roll(low, 64), high)

    for x in range(NX):
        for z in range(3):
            halo[x * 3 + z] = sh.y_up(image[at(x, 0, z)])
    for x in range(NX):
        for y in range(3):
            halo[36 + x * 3 + y] = sh.z_up(image[at(x, y, 0)])
    for k in range(PLANE):
        halo[144 + k] = sh.x_swap(image[k])
    for x, y, z in cells:
        t = at(x, y, z)
        here = image[t]
        ahead = image[t + PLANE] if x < NX - 1 else halo[144 + y * 3 + z]
        face[t] = (here + ahead) * 0.5
        ahead = image[t + 3] if y < 2 else halo[x * 3 + z]
        face[CELLS + t] = (here + ahead) * 0.5
        ahead = image[t + 1] if z < 2 else halo[36 + x * 3 + y]
        face[2 * CELLS + t] = (here + ahead) * 0.5
    for x in range(NX):
        for z in range(3):
            low_face[x * 3 + z] = sh.y_down(face[CELLS + at(x, 2, z)])
    for x in range(NX):
        for y in range(3):
            low_face[36 + x * 3 + y] = sh.z_down(face[2 * CELLS + at(x, y, 2)])
    for k in range(PLANE):
        low_face[72 + k] = sh.x_swap(face[at(NX - 1, 0, 0) + k])

    zero = jnp.zeros((8, 128), F32)
    norms = [zero] * 3
    means = [zero] * 3
    for x, y, z in cells:
        t = at(x, y, z)
        back = [
            face[t - PLANE] if x > 0 else low_face[72 + y * 3 + z],
            face[CELLS + t - 3] if y > 0 else low_face[x * 3 + z],
            face[2 * CELLS + t - 1] if z > 0 else low_face[36 + x * 3 + y],
        ]
        for c in range(3):
            here = face[c * CELLS + t]
            value = here - back[c]
            rhs[c * CELLS + t] = value
            remain[c * CELLS + t] = value
            direct[c * CELLS + t] = zero
            fluct[c * CELLS + t] = zero
            norms[c] = norms[c] + value * value
            means[c] = means[c] + here

    sub = lax.broadcasted_iota(jnp.int32, (8, 128), 0)
    counts = jnp.zeros((8, 128), jnp.int32)
    for k in range(EZ):
        counts = jnp.where(sub == k, counts_ref[k], counts)

    def update(c, alpha, beta):
        base, edge = c * CELLS, c * HALO
        for first in range(0, NX, CHUNK):
            span = range(first, first + CHUNK)
            plane = {}
            for x in span:
                for k in range(PLANE):
                    t = base + x * PLANE + k
                    old = direct[t]
                    fluct[t] = fluct[t] + alpha * old
                    plane[x, k] = remain[t] + beta * old
                    direct[t] = plane[x, k]
                yield
            for x in span:
                for z in range(3):
                    halo[edge + x * 3 + z] = sh.y_up(plane[x, z])
            for x in span:
                for z in range(3):
                    halo[edge + 72 + x * 3 + z] = sh.y_down(plane[x, 6 + z])
            for x in span:
                for y in range(3):
                    halo[edge + 36 + x * 3 + y] = sh.z_up(plane[x, 3 * y])
            for x in span:
                for y in range(3):
                    halo[edge + 108 + x * 3 + y] = sh.z_down(plane[x, 3 * y + 2])
            if first == 0:
                for k in range(PLANE):
                    halo[edge + 144 + k] = sh.x_swap(plane[0, k])
            if first + CHUNK == NX:
                for k in range(PLANE):
                    halo[edge + 153 + k] = sh.x_swap(plane[NX - 1, k])

    def stencil(c, box):
        base, edge = c * CELLS, c * HALO
        acc = zero
        here = [direct[base + k] for k in range(PLANE)]
        before = [low_face[72 + k] * (halo[edge + 153 + k] - here[k]) for k in range(PLANE)]
        for x in range(NX):
            if x < NX - 1:
                ahead = [direct[base + (x + 1) * PLANE + k] for k in range(PLANE)]
            else:
                ahead = [halo[edge + 144 + k] for k in range(PLANE)]
            for y in range(3):
                if y == 0:
                    flux_y = [low_face[x * 3 + z] * (halo[edge + 72 + x * 3 + z] - here[z]) for z in range(3)]
                flux_z = low_face[36 + x * 3 + y] * (halo[edge + 108 + x * 3 + y] - here[3 * y])
                for z in range(3):
                    k = 3 * y + z
                    t = x * PLANE + k
                    v = here[k]
                    next_x = face[t] * (v - ahead[k])
                    up = here[k + 3] if y < 2 else halo[edge + x * 3 + z]
                    next_y = face[CELLS + t] * (v - up)
                    up = here[k + 1] if z < 2 else halo[edge + 36 + x * 3 + y]
                    next_z = face[2 * CELLS + t] * (v - up)
                    out = (next_x - before[k]) + ((next_y - flux_y[z]) + (next_z - flux_z))
                    image[base + t] = out
                    acc = acc + v * out
                    before[k], flux_y[z], flux_z = next_x, next_y, next_z
            here = ahead
            yield
        box.append(acc)

    def descend(c, alpha, box):
        acc = zero
        for x in range(NX):
            for t in range(c * CELLS + x * PLANE, c * CELLS + (x + 1) * PLANE):
                value = remain[t] - alpha * image[t]
                remain[t] = value
                acc = acc + value * value
            yield
        box.append(acc)

    def together(*parts):
        parts = list(parts)
        while parts:
            for part in list(parts):
                if next(part, part) is part:
                    parts.remove(part)

    def sweep(index, carry):
        norm, alpha, beta, last = carry
        live = index < counts
        box = []
        together(update(1, alpha[1], beta[1]), stencil(0, box))
        step_0 = jnp.where(live, norm[0] / total(box[0]), 0.0)
        norm_2 = total(last)
        together(update(2, alpha[2], norm_2 / norm[2]), stencil(1, box))
        step_1 = jnp.where(live, norm[1] / total(box[1]), 0.0)
        together(stencil(2, box), descend(0, step_0, box))
        acc_2, acc_0 = (box[2], box[3])
        step_2 = jnp.where(live, norm_2 / total(acc_2), 0.0)
        norm_0 = total(acc_0)
        together(descend(1, step_1, box))
        norm_1 = total(box[4])
        together(descend(2, step_2, box))
        together(update(0, step_0, norm_0 / norm[0]))
        return (norm_0, norm_1, norm_2), (step_0, step_1, step_2), (zero, norm_1 / norm[1]), box[5]

    norm = tuple(total(v) for v in norms)
    together(update(0, zero, zero))
    first = (norm, (zero,) * 3, (zero, zero), jnp.where(lane_iota() == 0, norm[2], 0.0))
    norm, alpha, _, _ = lax.fori_loop(0, MICRO_MAX, sweep, first)

    inner = [[zero] * 3 for _ in range(3)]
    for t in range(CELLS):
        for c in range(3):
            value = fluct[c * CELLS + t]
            if c > 0:
                value = value + alpha[c] * direct[c * CELLS + t]
                fluct[c * CELLS + t] = value
            for d in range(3):
                inner[d][c] = inner[d][c] + value * rhs[d * CELLS + t]
    scale = 1.0 / (VOX * YZ)
    tangent = [
        [(total(means[d] - inner[d][c]) if d == c else -total(inner[d][c])) * scale for c in range(3)]
        for d in range(3)
    ]
    lane = lane_iota()
    for d in range(3):
        for c in range(3):
            spread = jnp.sum(jnp.where(sub == (lane & 7), tangent[d][c], 0.0), axis=0, keepdims=True)
            tangent_ref[d, c] = spread[:, 0:EZ]

    slot = lane >> 3
    message = jnp.where(slot == 0, tangent[0][0], jnp.where(slot == 1, tangent[1][1], tangent[2][2]))
    message = jnp.where((sub == (lane & 7)) & (slot < 3), message, 0.0)
    message = jnp.sum(message, axis=0, keepdims=True)
    low = lax.broadcasted_iota(jnp.int32, (1, 128), 1)
    for k in range(EZ):
        message = jnp.where(low == 24 + k, current_ref[k], message)
        message = jnp.where(low == 32 + k, load_ref[k], message)
    packed[...] = message
    pl.semaphore_wait(barrier, cols + rows - 2)

    x_at, z_at = col_at // 8, lax.rem(col_at, 8)
    y_at, core_at = row_at // 2, lax.rem(row_at, 2)

    def hops(steps, lengths):
        return sum(min(step, length - step) for step, length in zip(steps, lengths))

    def along_col(s, dx, dz):
        return pltpu.make_async_remote_copy(
            src_ref=packed,
            dst_ref=grid_ref.at[row_at, pl.ds(col_at, 1)],
            send_sem=send_a.at[s],
            recv_sem=recv_a.at[s],
            device_id=(row_at, lax.rem(x_at + dx, 4) * 8 + lax.rem(z_at + dz, 8)),
            device_id_type=MESH,
        )

    def along_row(s, dy, dc):
        return pltpu.make_async_remote_copy(
            src_ref=grid_ref.at[row_at],
            dst_ref=grid_ref.at[row_at],
            send_sem=send_b.at[s],
            recv_sem=recv_b.at[s],
            device_id=(lax.rem(y_at + dy, 4) * 2 + lax.rem(core_at + dc, 2), col_at),
            device_id_type=MESH,
        )

    col_steps = [(dx, dz) for dx in range(4) for dz in range(8) if dx or dz]
    col_steps.sort(key=lambda steps: -hops(steps, (4, 8)))
    row_steps = [(dy, dc) for dy in range(4) for dc in range(2) if dy or dc]
    row_steps.sort(key=lambda steps: -hops(steps, (4, 2)))
    col_copies = [along_col(s, *steps) for s, steps in enumerate(col_steps)]
    row_copies = [along_row(s, *steps) for s, steps in enumerate(row_steps)]

    for copy in col_copies:
        copy.start()
    grid_ref[row_at, pl.ds(col_at, 1), :] = message

    for c in range(3):
        for x in range(NX):
            for j in range(5):
                first = fluct[c * CELLS + x * PLANE + 2 * j]
                second = fluct[c * CELLS + x * PLANE + 2 * j + 1] if j < 4 else zero
                stage[j, pl.ds(c * ROWS + x, 8, stride=VOX), :] = jnp.where(sh.low, first, roll(second, 64))
                stage[j, pl.ds(c * ROWS + x + NX, 8, stride=VOX), :] = jnp.where(sh.low, roll(first, 64), second)
    whole = jnp.concatenate([stage[j, 0 : 3 * ROWS, :] for j in range(4)] + [stage[4, 0 : 3 * ROWS, 0:64]], axis=1)
    parts = jnp.concatenate(pieces(whole, 2), axis=0)
    moved = lax.dot_general(parts, perm[...], (((1,), (1,)), ((), ())), preferred_element_type=F32)
    moved = moved[3 * ROWS :] + moved[: 3 * ROWS]
    for c in range(3):
        states[:, c, :, :] = moved[c * ROWS : (c + 1) * ROWS].reshape(EZ, VOX, YZ)
    out = pltpu.make_async_copy(states, states_ref, out_sem)
    out.start()
    for copy in col_copies:
        copy.wait_recv()
    for copy in row_copies:
        copy.start()
    for copy in col_copies:
        copy.wait_send()
    for copy in row_copies:
        copy.wait()
    out.wait()


def heavy(phases, grain, phase_cond, counts, current, load):
    smem = pl.BlockSpec(memory_space=pltpu.SMEM)
    vmem = pl.BlockSpec(memory_space=pltpu.VMEM)
    field = pltpu.VMEM((3 * CELLS, 8, 128), F32)
    return pl.pallas_call(
        heavy_kernel,
        out_shape=(
            jax.ShapeDtypeStruct((EZ, 3, VOX, YZ), F32),
            jax.ShapeDtypeStruct((3, 3, 1, EZ), F32),
            jax.ShapeDtypeStruct((8, 32, 128), F32),
        ),
        in_specs=[smem, smem, smem, smem, vmem, vmem],
        out_specs=(pl.BlockSpec(memory_space=pl.ANY), vmem, vmem),
        scratch_shapes=[
            pltpu.VMEM((YZ, YZ), BF16),
            pltpu.VMEM((5, 3 * ROWS, 128), F32),
            field,
            pltpu.VMEM((81, 8, 128), F32),
            field, field, field, field, field,
            pltpu.VMEM((3 * HALO, 8, 128), F32),
            pltpu.VMEM((1, 128), F32),
            pltpu.VMEM((EZ, 3, VOX, YZ), F32),
            pltpu.SemaphoreType.DMA((32,)),
            pltpu.SemaphoreType.DMA((32,)),
            pltpu.SemaphoreType.DMA((8,)),
            pltpu.SemaphoreType.DMA((8,)),
            pltpu.SemaphoreType.DMA,
        ],
        compiler_params=pltpu.CompilerParams(
            vmem_limit_bytes=62 * 1024 * 1024, collective_id=0, has_side_effects=True
        ),
        name="micro",
    )(phase_cond, counts, current, load, phases, grain)


def coarse_kernel(
    grid, states_in, tangent_in, states_ref, tangent_ref, increment_ref, residual_ref, states, in_sem, out_sem
):
    cols = 32
    i, j = lax.axis_index("row"), lax.axis_index("col")
    inward = [pltpu.make_async_copy(states_in.at[e], states.at[e], in_sem.at[e]) for e in range(EZ)]
    outward = [pltpu.make_async_copy(states.at[e], states_ref.at[e], out_sem.at[e]) for e in range(EZ)]
    for copy in inward:
        copy.start()
    tangent_ref[...] = tangent_in[...]

    lane = lane_iota()
    slot = lane >> 3
    sub = lax.broadcasted_iota(jnp.int32, (8, 128), 0)
    fields = [[jnp.zeros((8, 128), F32)] * 2 for _ in range(5)]
    for col in range(cols):
        at_col = grid[:, col, :]
        half, place = divmod(col, 16)
        for f in range(5):
            spun = roll(at_col, (place - f) * 8)
            fields[f][half] = jnp.where(slot == place, spun, fields[f][half])
    kx, ky, kz, current, load = fields
    for before, after in zip(inward, outward):
        before.wait()
        after.start()

    def ahead_y(v):
        spun = [roll(part, -8) for part in v]
        return [jnp.where(slot == 15, spun[1], spun[0]), spun[1]]

    def back_y(v):
        spun = [roll(part, 8) for part in v]
        return [spun[0], jnp.where(slot == 0, spun[0], spun[1])]

    def ahead_z(v):
        return [roll(part, -1) for part in v]

    def back_z(v):
        return [roll(part, 1) for part in v]

    def ahead_x(v):
        return [pltpu.roll(part, 7, 0) for part in v]

    def back_x(v):
        return [pltpu.roll(part, 1, 0) for part in v]

    k_in = lane & 7
    never = lane < 0
    outside = [
        ([sub == 7] * 2, [sub == 0] * 2),
        ([never, slot == 15], [slot == 0, never]),
        ([k_in == 7] * 2, [k_in == 0] * 2),
    ]
    moves = [(ahead_x, back_x), (ahead_y, back_y), (ahead_z, back_z)]
    weights = []
    centre = [jnp.zeros((8, 128), F32)] * 2
    for (pair, masks), k in zip(zip(moves, outside), (kx, ky, kz)):
        for move, mask in zip(pair, masks):
            near = move(k)
            cond = [0.5 * (k[h] + jnp.where(mask[h], 0.0, near[h])) for h in range(2)]
            centre = [centre[h] + cond[h] for h in range(2)]
            weights.append((move, [jnp.where(mask[h], 0.0, cond[h]) for h in range(2)]))

    def apply(v):
        out = [centre[h] * v[h] for h in range(2)]
        for move, weight in weights:
            near = move(v)
            out = [out[h] - weight[h] * near[h] for h in range(2)]
        return out

    def dot(a, b):
        both = a[0] * b[0] + a[1] * b[1]
        both = jnp.sum(both, axis=0, keepdims=True)
        return jnp.broadcast_to(jnp.sum(both, axis=1, keepdims=True), (8, 128))

    image = apply(current)
    residual = [load[h] - image[h] for h in range(2)]
    increment = [jnp.zeros((8, 128), F32)] * 2
    applied = apply(residual)
    norm, curve = dot(residual, residual), dot(residual, applied)
    step = norm / curve
    direction, image = residual, applied
    for iteration in range(MACRO_ITERS):
        increment = [increment[h] + step * direction[h] for h in range(2)]
        residual = [residual[h] - step * image[h] for h in range(2)]
        if iteration == MACRO_ITERS - 1:
            break
        applied = apply(residual)
        fresh, curve = dot(residual, residual), dot(residual, applied)
        ratio = fresh / norm
        step = fresh / (curve - ratio * (fresh / step))
        norm = fresh
        direction = [residual[h] + ratio * direction[h] for h in range(2)]
        image = [applied[h] + ratio * image[h] for h in range(2)]

    place = lax.rem(j, 16)

    def own(v):
        part = jnp.where(j < 16, v[0], v[1])
        part = jnp.where((sub == i) & (slot == place), part, 0.0)
        part = jnp.broadcast_to(jnp.sum(part, axis=0, keepdims=True), (8, 128))
        spun = pltpu.roll(part, lax.rem(128 - place * 8, 128), 1)
        return spun[0:1, 0:EZ]

    increment_ref[...] = own(increment)
    residual_ref[...] = own(residual)
    for copy in outward:
        copy.wait()


def coarse(grid, states, tangent):
    vmem = pl.BlockSpec(memory_space=pltpu.VMEM)
    hbm = pl.BlockSpec(memory_space=pl.ANY)
    out = jax.ShapeDtypeStruct((1, EZ), F32)
    return pl.pallas_call(
        coarse_kernel,
        out_shape=(
            jax.ShapeDtypeStruct((EZ, 3, VOX, YZ), F32),
            jax.ShapeDtypeStruct((3, 3, 1, EZ), F32),
            out,
            out,
        ),
        in_specs=[vmem, hbm, vmem],
        out_specs=(hbm, vmem, vmem, vmem),
        scratch_shapes=[
            pltpu.VMEM((EZ, 3, VOX, YZ), F32),
            pltpu.SemaphoreType.DMA((EZ,)),
            pltpu.SemaphoreType.DMA((EZ,)),
        ],
        name="coarse",
    )(grid, states, tangent)


def shards(phases, grain, phase_cond, micro_counts, current, load):
    states, tangent, grid = heavy(
        phases.reshape(EZ, VOX, YZ), grain.reshape(EZ, VOX, YZ), phase_cond,
        micro_counts.reshape(EZ), current.reshape(EZ), load.reshape(EZ),
    )
    states, tangent, increment, residual = coarse(grid, states, tangent)
    return (
        states.reshape(1, 1, EZ, 3, VOX, YZ),
        jnp.moveaxis(tangent, 3, 0).reshape(1, 1, EZ, 3, 3),
        increment.reshape(1, 1, EZ),
        residual.reshape(1, 1, EZ),
    )


def solution(mesh):
    in_specs = (
        P("row", "col", None, None, None),
        P("row", "col", None, None, None),
        P(),
        P("row", "col", None),
        P("row", "col", None),
        P("row", "col", None),
    )
    out_specs = (
        P("row", "col", None, None, None, None),
        P("row", "col", None, None, None),
        P("row", "col", None),
        P("row", "col", None),
    )
    return jax.shard_map(shards, mesh=mesh, in_specs=in_specs, out_specs=out_specs, check_vma=False)
```

```python
import functools

import jax
import jax.numpy as jnp
from jax import lax
from jax.experimental import pallas as pl
from jax.experimental.pallas import tpu as pltpu
from jax.sharding import PartitionSpec as P

VOX = 24
YZ = 576
PHASES = 3
EZ = 8
MICRO_MAX = 12
MACRO_ITERS = 8
NX = 12
PLANE = 9
CELLS = NX * PLANE
ROWS = EZ * VOX
HALO = 162
CHUNK = 3
F32 = jnp.float32
BF16 = jnp.bfloat16
MESH = pl.DeviceIdType.MESH


def lane_iota():
    return lax.broadcasted_iota(jnp.int32, (8, 128), 1)


def roll(v, shift):
    return pltpu.roll(v, shift % 128, 1)


class Shifts:
    def __init__(self):
        lane = lane_iota()
        ys = (lane >> 3) & 7
        zs = lane & 7
        self.y_up = self.gather(jnp.where(ys == 7, lane - 56, lane + 8))
        self.y_down = self.gather(jnp.where(ys == 0, lane + 56, lane - 8))
        self.z_up = self.gather(jnp.where(zs == 7, lane - 7, lane + 1))
        self.z_down = self.gather(jnp.where(zs == 0, lane + 7, lane - 1))
        self.low = lane < 64

    def gather(self, source):
        return lambda v: jnp.take_along_axis(v, source, axis=1, mode="promise_in_bounds")

    def x_swap(self, v):
        return roll(v, 64)


def pieces(v, count):
    out = []
    for _ in range(count - 1):
        part = v.astype(BF16)
        out.append(part)
        v = v - part.astype(F32)
    out.append(v.astype(BF16))
    return out


def permutation():
    col = lax.broadcasted_iota(jnp.int32, (YZ, YZ), 1)
    row = lax.broadcasted_iota(jnp.int32, (YZ, YZ), 0)
    group = col >> 6
    y_in = (group * 11) >> 5
    z_in = group - 3 * y_in
    source = (((col >> 3) & 7) * 3 + y_in) * VOX + (col & 7) * 3 + z_in
    return jnp.where(row == source, 1.0, 0.0).astype(BF16)


def total(v):
    return jnp.broadcast_to(jnp.sum(v, axis=1, keepdims=True), (8, 128))


def gathered_rows(inbox, slot, sub):
    spans = [pltpu.roll(inbox[8 * q : 8 * q + 8, :], q % 2 * 64, 1, stride=8, stride_axis=0) for q in range(4)]
    block = [jnp.zeros((8, 128), F32)] * 2
    for f in range(5):
        for h in range(2):
            both = jnp.zeros((8, 128), F32)
            for q in (0, 1):
                both = both + jnp.where(slot == ((8 * q + sub + f) & 15), spans[2 * h + q], 0.0)
            row = 2 * f + h
            line = jnp.broadcast_to(jnp.sum(both, axis=0, keepdims=True), (8, 128))
            block[row // 8] = jnp.where(sub == row % 8, line, block[row // 8])
    return jnp.concatenate(block, axis=0)


def heavy_kernel(
    cond_ref, counts_ref, current_ref, load_ref, phases_in, grain_in,
    states_ref, tangent_ref, grid_ref,
    perm, stage, face, low_face, rhs, fluct, remain, direct, image, halo, packed, inbox, states, phases_ref, grain_ref,
    send_a, recv_a, send_b, recv_b, out_sem, phases_sem, grain_sem,
):
    inputs = [
        pltpu.make_async_copy(phases_in, phases_ref, phases_sem),
        pltpu.make_async_copy(grain_in, grain_ref, grain_sem),
    ]
    for copy in inputs:
        copy.start()
    rows, cols = 8, 32
    row_at, col_at = lax.axis_index("row"), lax.axis_index("col")
    barrier = pltpu.get_barrier_semaphore()

    def greet_col(s, _):
        pl.semaphore_signal(barrier, inc=1, device_id=(row_at, lax.rem(col_at + s, cols)), device_id_type=MESH)
        return 0

    def greet_row(s, _):
        pl.semaphore_signal(barrier, inc=1, device_id=(lax.rem(row_at + s, rows), col_at), device_id_type=MESH)
        return 0

    lax.fori_loop(1, cols, greet_col, 0)
    lax.fori_loop(1, rows, greet_row, 0)

    sh = Shifts()
    cells = [(x, y, z) for x in range(NX) for y in range(3) for z in range(3)]

    def at(x, y, z):
        return x * PLANE + y * 3 + z

    perm[...] = permutation()
    for copy in inputs:
        copy.wait()
    phases = phases_ref[...].reshape(ROWS, YZ)
    conduct = jnp.zeros((ROWS, YZ), F32)
    for phase_id in range(PHASES):
        conduct = jnp.where(phases == phase_id, cond_ref[phase_id], conduct)
    conduct = conduct * grain_ref[...].reshape(ROWS, YZ)
    parts = jnp.concatenate(pieces(conduct, 3), axis=0)
    moved = jnp.dot(parts, perm[...], preferred_element_type=F32)
    moved = (moved[2 * ROWS :] + moved[ROWS : 2 * ROWS]) + moved[:ROWS]
    for j in range(4):
        stage[j, 0:ROWS, :] = moved[:, 128 * j : 128 * j + 128]
    stage[4, 0:ROWS, 0:64] = moved[:, 512:576]

    for x in range(NX):
        for j in range(5):
            low = stage[j, pl.ds(x, 8, stride=VOX), :]
            high = stage[j, pl.ds(x + NX, 8, stride=VOX), :]
            image[x * PLANE + 2 * j] = jnp.where(sh.low, low, roll(high, 64))
            if j < 4:
                image[x * PLANE + 2 * j + 1] = jnp.where(sh.low, roll(low, 64), high)

    for x in range(NX):
        for z in range(3):
            halo[x * 3 + z] = sh.y_up(image[at(x, 0, z)])
    for x in range(NX):
        for y in range(3):
            halo[36 + x * 3 + y] = sh.z_up(image[at(x, y, 0)])
    for k in range(PLANE):
        halo[144 + k] = sh.x_swap(image[k])
    for x, y, z in cells:
        t = at(x, y, z)
        here = image[t]
        ahead = image[t + PLANE] if x < NX - 1 else halo[144 + y * 3 + z]
        face[t] = (here + ahead) * 0.5
        ahead = image[t + 3] if y < 2 else halo[x * 3 + z]
        face[CELLS + t] = (here + ahead) * 0.5
        ahead = image[t + 1] if z < 2 else halo[36 + x * 3 + y]
        face[2 * CELLS + t] = (here + ahead) * 0.5
    for x in range(NX):
        for z in range(3):
            low_face[x * 3 + z] = sh.y_down(face[CELLS + at(x, 2, z)])
    for x in range(NX):
        for y in range(3):
            low_face[36 + x * 3 + y] = sh.z_down(face[2 * CELLS + at(x, y, 2)])
    for k in range(PLANE):
        low_face[72 + k] = sh.x_swap(face[at(NX - 1, 0, 0) + k])

    zero = jnp.zeros((8, 128), F32)
    norms = [zero] * 3
    means = [zero] * 3
    for x, y, z in cells:
        t = at(x, y, z)
        back = [
            face[t - PLANE] if x > 0 else low_face[72 + y * 3 + z],
            face[CELLS + t - 3] if y > 0 else low_face[x * 3 + z],
            face[2 * CELLS + t - 1] if z > 0 else low_face[36 + x * 3 + y],
        ]
        for c in range(3):
            here = face[c * CELLS + t]
            value = here - back[c]
            rhs[c * CELLS + t] = value
            remain[c * CELLS + t] = value
            direct[c * CELLS + t] = zero
            fluct[c * CELLS + t] = zero
            norms[c] = norms[c] + value * value
            means[c] = means[c] + here

    sub = lax.broadcasted_iota(jnp.int32, (8, 128), 0)
    counts = jnp.zeros((8, 128), jnp.int32)
    for k in range(EZ):
        counts = jnp.where(sub == k, counts_ref[k], counts)

    def update(c, alpha, beta):
        base, edge = c * CELLS, c * HALO
        for first in range(0, NX, CHUNK):
            span = range(first, first + CHUNK)
            plane = {}
            for x in span:
                for k in range(PLANE):
                    t = base + x * PLANE + k
                    old = direct[t]
                    fluct[t] = fluct[t] + alpha * old
                    plane[x, k] = remain[t] + beta * old
                    direct[t] = plane[x, k]
                yield
            for x in span:
                for z in range(3):
                    halo[edge + x * 3 + z] = sh.y_up(plane[x, z])
            for x in span:
                for z in range(3):
                    halo[edge + 72 + x * 3 + z] = sh.y_down(plane[x, 6 + z])
            for x in span:
                for y in range(3):
                    halo[edge + 36 + x * 3 + y] = sh.z_up(plane[x, 3 * y])
            for x in span:
                for y in range(3):
                    halo[edge + 108 + x * 3 + y] = sh.z_down(plane[x, 3 * y + 2])
            if first == 0:
                for k in range(PLANE):
                    halo[edge + 144 + k] = sh.x_swap(plane[0, k])
            if first + CHUNK == NX:
                for k in range(PLANE):
                    halo[edge + 153 + k] = sh.x_swap(plane[NX - 1, k])

    def stencil(c, box):
        base, edge = c * CELLS, c * HALO
        acc = zero
        here = [direct[base + k] for k in range(PLANE)]
        before = [low_face[72 + k] * (halo[edge + 153 + k] - here[k]) for k in range(PLANE)]
        for x in range(NX):
            if x < NX - 1:
                ahead = [direct[base + (x + 1) * PLANE + k] for k in range(PLANE)]
            else:
                ahead = [halo[edge + 144 + k] for k in range(PLANE)]
            for y in range(3):
                if y == 0:
                    flux_y = [low_face[x * 3 + z] * (halo[edge + 72 + x * 3 + z] - here[z]) for z in range(3)]
                flux_z = low_face[36 + x * 3 + y] * (halo[edge + 108 + x * 3 + y] - here[3 * y])
                for z in range(3):
                    k = 3 * y + z
                    t = x * PLANE + k
                    v = here[k]
                    next_x = face[t] * (v - ahead[k])
                    up = here[k + 3] if y < 2 else halo[edge + x * 3 + z]
                    next_y = face[CELLS + t] * (v - up)
                    up = here[k + 1] if z < 2 else halo[edge + 36 + x * 3 + y]
                    next_z = face[2 * CELLS + t] * (v - up)
                    out = (next_x - before[k]) + ((next_y - flux_y[z]) + (next_z - flux_z))
                    image[base + t] = out
                    acc = acc + v * out
                    before[k], flux_y[z], flux_z = next_x, next_y, next_z
            here = ahead
            yield
        box.append(acc)

    def descend(c, alpha, box):
        acc = zero
        for x in range(NX):
            for t in range(c * CELLS + x * PLANE, c * CELLS + (x + 1) * PLANE):
                value = remain[t] - alpha * image[t]
                remain[t] = value
                acc = acc + value * value
            yield
        box.append(acc)

    def together(*parts):
        parts = list(parts)
        while parts:
            for part in list(parts):
                if next(part, part) is part:
                    parts.remove(part)

    def sweep(index, carry):
        norm, alpha, beta, last = carry
        live = index < counts
        box = []
        together(update(1, alpha[1], beta[1]), stencil(0, box))
        step_0 = jnp.where(live, norm[0] / total(box[0]), 0.0)
        norm_2 = total(last)
        together(update(2, alpha[2], norm_2 / norm[2]), stencil(1, box))
        step_1 = jnp.where(live, norm[1] / total(box[1]), 0.0)
        together(stencil(2, box), descend(0, step_0, box))
        acc_2, acc_0 = (box[2], box[3])
        step_2 = jnp.where(live, norm_2 / total(acc_2), 0.0)
        norm_0 = total(acc_0)
        together(descend(1, step_1, box))
        norm_1 = total(box[4])
        together(descend(2, step_2, box))
        together(update(0, step_0, norm_0 / norm[0]))
        return (norm_0, norm_1, norm_2), (step_0, step_1, step_2), (zero, norm_1 / norm[1]), box[5]

    norm = tuple(total(v) for v in norms)
    together(update(0, zero, zero))
    first = (norm, (zero,) * 3, (zero, zero), jnp.where(lane_iota() == 0, norm[2], 0.0))
    norm, alpha, _, _ = lax.fori_loop(0, MICRO_MAX, sweep, first)

    inner = [[zero] * 3 for _ in range(3)]
    for t in range(CELLS):
        for c in range(3):
            value = fluct[c * CELLS + t]
            if c > 0:
                value = value + alpha[c] * direct[c * CELLS + t]
                fluct[c * CELLS + t] = value
            for d in range(3):
                inner[d][c] = inner[d][c] + value * rhs[d * CELLS + t]
    scale = 1.0 / (VOX * YZ)
    tangent = [
        [(total(means[d] - inner[d][c]) if d == c else -total(inner[d][c])) * scale for c in range(3)]
        for d in range(3)
    ]
    lane = lane_iota()
    for d in range(3):
        for c in range(3):
            spread = jnp.sum(jnp.where(sub == (lane & 7), tangent[d][c], 0.0), axis=0, keepdims=True)
            tangent_ref[d, c] = spread[:, 0:EZ]

    slot = lane >> 3
    message = jnp.where(slot == 0, tangent[0][0], jnp.where(slot == 1, tangent[1][1], tangent[2][2]))
    message = jnp.where((sub == (lane & 7)) & (slot < 3), message, 0.0)
    message = jnp.sum(message, axis=0, keepdims=True)
    low = lax.broadcasted_iota(jnp.int32, (1, 128), 1)
    for k in range(EZ):
        message = jnp.where(low == 24 + k, current_ref[k], message)
        message = jnp.where(low == 32 + k, load_ref[k], message)
    packed[...] = message
    pl.semaphore_wait(barrier, cols + rows - 2)

    x_at, z_at = col_at // 8, lax.rem(col_at, 8)
    y_at, core_at = row_at // 2, lax.rem(row_at, 2)

    def hops(steps, lengths):
        return sum(min(step, length - step) for step, length in zip(steps, lengths))

    def along_col(s, dx, dz):
        return pltpu.make_async_remote_copy(
            src_ref=packed,
            dst_ref=inbox.at[pl.ds(col_at, 1)],
            send_sem=send_a.at[s],
            recv_sem=recv_a.at[s],
            device_id=(row_at, lax.rem(x_at + dx, 4) * 8 + lax.rem(z_at + dz, 8)),
            device_id_type=MESH,
        )

    def along_row(s, dy, dc):
        return pltpu.make_async_remote_copy(
            src_ref=grid_ref.at[row_at],
            dst_ref=grid_ref.at[row_at],
            send_sem=send_b.at[s],
            recv_sem=recv_b.at[s],
            device_id=(lax.rem(y_at + dy, 4) * 2 + lax.rem(core_at + dc, 2), col_at),
            device_id_type=MESH,
        )

    col_steps = [(dx, dz) for dx in range(4) for dz in range(8) if dx or dz]
    col_steps.sort(key=lambda steps: -hops(steps, (4, 8)))
    row_steps = [(dy, dc) for dy in range(4) for dc in range(2) if dy or dc]
    row_steps.sort(key=lambda steps: -hops(steps, (4, 2)))
    col_copies = [along_col(s, *steps) for s, steps in enumerate(col_steps)]
    row_copies = [along_row(s, *steps) for s, steps in enumerate(row_steps)]

    for copy in col_copies:
        copy.start()
    inbox[pl.ds(col_at, 1), :] = message

    for c in range(3):
        for x in range(NX):
            for j in range(5):
                first = fluct[c * CELLS + x * PLANE + 2 * j]
                second = fluct[c * CELLS + x * PLANE + 2 * j + 1] if j < 4 else zero
                stage[j, pl.ds(c * ROWS + x, 8, stride=VOX), :] = jnp.where(sh.low, first, roll(second, 64))
                stage[j, pl.ds(c * ROWS + x + NX, 8, stride=VOX), :] = jnp.where(sh.low, roll(first, 64), second)
    whole = jnp.concatenate([stage[j, 0 : 3 * ROWS, :] for j in range(4)] + [stage[4, 0 : 3 * ROWS, 0:64]], axis=1)
    parts = jnp.concatenate(pieces(whole, 2), axis=0)
    moved = lax.dot_general(parts, perm[...], (((1,), (1,)), ((), ())), preferred_element_type=F32)
    moved = moved[3 * ROWS :] + moved[: 3 * ROWS]
    for c in range(3):
        states[:, c, :, :] = moved[c * ROWS : (c + 1) * ROWS].reshape(EZ, VOX, YZ)
    out = pltpu.make_async_copy(states, states_ref, out_sem)
    out.start()
    for copy in col_copies:
        copy.wait_recv()
    grid_ref[row_at] = gathered_rows(inbox, slot, sub)
    for copy in row_copies:
        copy.start()
    for copy in col_copies:
        copy.wait_send()
    for copy in row_copies:
        copy.wait()
    out.wait()


def heavy(phases, grain, phase_cond, counts, current, load):
    smem = pl.BlockSpec(memory_space=pltpu.SMEM)
    vmem = pl.BlockSpec(memory_space=pltpu.VMEM)
    hbm = pl.BlockSpec(memory_space=pl.ANY)
    field = pltpu.VMEM((3 * CELLS, 8, 128), F32)
    return pl.pallas_call(
        heavy_kernel,
        out_shape=(
            jax.ShapeDtypeStruct((EZ, 3, VOX, YZ), F32),
            jax.ShapeDtypeStruct((3, 3, 1, EZ), F32),
            jax.ShapeDtypeStruct((8, 16, 128), F32),
        ),
        in_specs=[smem, smem, smem, smem, hbm, hbm],
        out_specs=(hbm, vmem, vmem),
        scratch_shapes=[
            pltpu.VMEM((YZ, YZ), BF16),
            pltpu.VMEM((5, 3 * ROWS, 128), F32),
            field,
            pltpu.VMEM((81, 8, 128), F32),
            field, field, field, field, field,
            pltpu.VMEM((3 * HALO, 8, 128), F32),
            pltpu.VMEM((1, 128), F32),
            pltpu.VMEM((32, 128), F32),
            pltpu.VMEM((EZ, 3, VOX, YZ), F32),
            pltpu.VMEM((EZ, VOX, YZ), jnp.int32),
            pltpu.VMEM((EZ, VOX, YZ), F32),
            pltpu.SemaphoreType.DMA((32,)),
            pltpu.SemaphoreType.DMA((32,)),
            pltpu.SemaphoreType.DMA((8,)),
            pltpu.SemaphoreType.DMA((8,)),
            pltpu.SemaphoreType.DMA,
            pltpu.SemaphoreType.DMA,
            pltpu.SemaphoreType.DMA,
        ],
        compiler_params=pltpu.CompilerParams(
            vmem_limit_bytes=62 * 1024 * 1024, collective_id=0, has_side_effects=True
        ),
        name="micro",
    )(phase_cond, counts, current, load, phases, grain)


def coarse_kernel(
    grid, states_in, tangent_in, states_ref, tangent_ref, increment_ref, residual_ref, states, in_sem, out_sem
):
    i, j = lax.axis_index("row"), lax.axis_index("col")
    inward = [pltpu.make_async_copy(states_in.at[e], states.at[e], in_sem.at[e]) for e in range(EZ)]
    outward = [pltpu.make_async_copy(states.at[e], states_ref.at[e], out_sem.at[e]) for e in range(EZ)]
    for copy in inward:
        copy.start()
    tangent_ref[...] = tangent_in[...]

    lane = lane_iota()
    slot = lane >> 3
    sub = lax.broadcasted_iota(jnp.int32, (8, 128), 0)
    fields = [[roll(grid[:, 2 * f + h, :], -8 * f) for h in range(2)] for f in range(5)]
    kx, ky, kz, current, load = fields

    def ahead_y(v):
        spun = [roll(part, -8) for part in v]
        return [jnp.where(slot == 15, spun[1], spun[0]), spun[1]]

    def back_y(v):
        spun = [roll(part, 8) for part in v]
        return [spun[0], jnp.where(slot == 0, spun[0], spun[1])]

    def ahead_z(v):
        return [roll(part, -1) for part in v]

    def back_z(v):
        return [roll(part, 1) for part in v]

    def ahead_x(v):
        return [pltpu.roll(part, 7, 0) for part in v]

    def back_x(v):
        return [pltpu.roll(part, 1, 0) for part in v]

    k_in = lane & 7
    never = lane < 0
    outside = [
        ([sub == 7] * 2, [sub == 0] * 2),
        ([never, slot == 15], [slot == 0, never]),
        ([k_in == 7] * 2, [k_in == 0] * 2),
    ]
    moves = [(ahead_x, back_x), (ahead_y, back_y), (ahead_z, back_z)]
    weights = []
    centre = [jnp.zeros((8, 128), F32)] * 2
    for (pair, masks), k in zip(zip(moves, outside), (kx, ky, kz)):
        for move, mask in zip(pair, masks):
            near = move(k)
            cond = [0.5 * (k[h] + jnp.where(mask[h], 0.0, near[h])) for h in range(2)]
            centre = [centre[h] + cond[h] for h in range(2)]
            weights.append((move, [jnp.where(mask[h], 0.0, cond[h]) for h in range(2)]))

    def apply(v):
        out = [centre[h] * v[h] for h in range(2)]
        for move, weight in weights:
            near = move(v)
            out = [out[h] - weight[h] * near[h] for h in range(2)]
        return out

    def dot(a, b):
        both = a[0] * b[0] + a[1] * b[1]
        both = jnp.sum(both, axis=0, keepdims=True)
        return jnp.broadcast_to(jnp.sum(both, axis=1, keepdims=True), (8, 128))

    image = apply(current)
    residual = [load[h] - image[h] for h in range(2)]
    increment = [jnp.zeros((8, 128), F32)] * 2
    applied = apply(residual)
    norm, curve = dot(residual, residual), dot(residual, applied)
    step = norm / curve
    direction, image = residual, applied
    for iteration in range(MACRO_ITERS):
        increment = [increment[h] + step * direction[h] for h in range(2)]
        residual = [residual[h] - step * image[h] for h in range(2)]
        if iteration == 0:
            for before, after in zip(inward, outward):
                before.wait()
                after.start()
        if iteration == MACRO_ITERS - 1:
            break
        applied = apply(residual)
        fresh, curve = dot(residual, residual), dot(residual, applied)
        ratio = fresh / norm
        step = fresh / (curve - ratio * (fresh / step))
        norm = fresh
        direction = [residual[h] + ratio * direction[h] for h in range(2)]
        image = [applied[h] + ratio * image[h] for h in range(2)]

    place = lax.rem(j, 16)

    def own(v):
        part = jnp.where(j < 16, v[0], v[1])
        part = jnp.where((sub == i) & (slot == place), part, 0.0)
        part = jnp.broadcast_to(jnp.sum(part, axis=0, keepdims=True), (8, 128))
        spun = pltpu.roll(part, lax.rem(128 - place * 8, 128), 1)
        return spun[0:1, 0:EZ]

    increment_ref[...] = own(increment)
    residual_ref[...] = own(residual)
    for copy in outward:
        copy.wait()


def coarse(grid, states, tangent):
    vmem = pl.BlockSpec(memory_space=pltpu.VMEM)
    hbm = pl.BlockSpec(memory_space=pl.ANY)
    out = jax.ShapeDtypeStruct((1, EZ), F32)
    return pl.pallas_call(
        coarse_kernel,
        out_shape=(
            jax.ShapeDtypeStruct((EZ, 3, VOX, YZ), F32),
            jax.ShapeDtypeStruct((3, 3, 1, EZ), F32),
            out,
            out,
        ),
        in_specs=[vmem, hbm, vmem],
        out_specs=(hbm, vmem, vmem, vmem),
        scratch_shapes=[
            pltpu.VMEM((EZ, 3, VOX, YZ), F32),
            pltpu.SemaphoreType.DMA((EZ,)),
            pltpu.SemaphoreType.DMA((EZ,)),
        ],
        name="coarse",
    )(grid, states, tangent)


def shards(phases, grain, phase_cond, micro_counts, current, load):
    states, tangent, grid = heavy(
        phases.reshape(EZ, VOX, YZ), grain.reshape(EZ, VOX, YZ), phase_cond,
        micro_counts.reshape(EZ), current.reshape(EZ), load.reshape(EZ),
    )
    states, tangent, increment, residual = coarse(grid, states, tangent)
    return (
        states.reshape(1, 1, EZ, 3, VOX, YZ),
        jnp.moveaxis(tangent, 3, 0).reshape(1, 1, EZ, 3, 3),
        increment.reshape(1, 1, EZ),
        residual.reshape(1, 1, EZ),
    )


def solution(mesh):
    in_specs = (
        P("row", "col", None, None, None),
        P("row", "col", None, None, None),
        P(),
        P("row", "col", None),
        P("row", "col", None),
        P("row", "col", None),
    )
    out_specs = (
        P("row", "col", None, None, None, None),
        P("row", "col", None, None, None),
        P("row", "col", None),
        P("row", "col", None),
    )
    return jax.shard_map(shards, mesh=mesh, in_specs=in_specs, out_specs=out_specs, check_vma=False)
```

```python
import functools

import jax
import jax.numpy as jnp
from jax import lax
from jax.experimental import pallas as pl
from jax.experimental.pallas import tpu as pltpu
from jax.sharding import PartitionSpec as P

VOX = 24
YZ = 576
PHASES = 3
EZ = 8
MICRO_MAX = 12
MACRO_ITERS = 8
NX = 12
PLANE = 9
CELLS = NX * PLANE
ROWS = EZ * VOX
HALO = 162
CHUNK = 3
F32 = jnp.float32
BF16 = jnp.bfloat16
MESH = pl.DeviceIdType.MESH


def lane_iota():
    return lax.broadcasted_iota(jnp.int32, (8, 128), 1)


def roll(v, shift):
    return pltpu.roll(v, shift % 128, 1)


class Shifts:
    def __init__(self):
        lane = lane_iota()
        ys = (lane >> 3) & 7
        zs = lane & 7
        self.y_up = self.gather(jnp.where(ys == 7, lane - 56, lane + 8))
        self.y_down = self.gather(jnp.where(ys == 0, lane + 56, lane - 8))
        self.z_up = self.gather(jnp.where(zs == 7, lane - 7, lane + 1))
        self.z_down = self.gather(jnp.where(zs == 0, lane + 7, lane - 1))
        self.low = lane < 64

    def gather(self, source):
        return lambda v: jnp.take_along_axis(v, source, axis=1, mode="promise_in_bounds")

    def x_swap(self, v):
        return roll(v, 64)


def pieces(v, count):
    out = []
    for _ in range(count - 1):
        part = v.astype(BF16)
        out.append(part)
        v = v - part.astype(F32)
    out.append(v.astype(BF16))
    return out


def permutation():
    col = lax.broadcasted_iota(jnp.int32, (YZ, YZ), 1)
    row = lax.broadcasted_iota(jnp.int32, (YZ, YZ), 0)
    group = col >> 6
    y_in = (group * 11) >> 5
    z_in = group - 3 * y_in
    source = (((col >> 3) & 7) * 3 + y_in) * VOX + (col & 7) * 3 + z_in
    return jnp.where(row == source, 1.0, 0.0).astype(BF16)


def total(v):
    return jnp.broadcast_to(jnp.sum(v, axis=1, keepdims=True), (8, 128))


def gathered_rows(inbox, slot, sub):
    spans = [pltpu.roll(inbox[8 * q : 8 * q + 8, :], q % 2 * 64, 1, stride=8, stride_axis=0) for q in range(4)]
    block = [jnp.zeros((8, 128), F32)] * 2
    for f in range(5):
        for h in range(2):
            both = jnp.zeros((8, 128), F32)
            for q in (0, 1):
                both = both + jnp.where(slot == ((8 * q + sub + f) & 15), spans[2 * h + q], 0.0)
            row = 2 * f + h
            line = jnp.broadcast_to(jnp.sum(both, axis=0, keepdims=True), (8, 128))
            block[row // 8] = jnp.where(sub == row % 8, line, block[row // 8])
    return jnp.concatenate(block, axis=0)


def heavy_kernel(
    cond_ref, counts_ref, current_ref, load_ref, phases_in, grain_in,
    states_ref, tangent_ref, grid_ref,
    perm, stage, face, low_face, rhs, fluct, remain, direct, image, halo, packed, inbox, states, phases_ref, grain_ref,
    send_a, recv_a, send_b, recv_b, out_sem, phases_sem, grain_sem,
):
    inputs = [
        pltpu.make_async_copy(phases_in, phases_ref, phases_sem),
        pltpu.make_async_copy(grain_in, grain_ref, grain_sem),
    ]
    for copy in inputs:
        copy.start()
    rows, cols = 8, 32
    row_at, col_at = lax.axis_index("row"), lax.axis_index("col")
    barrier = pltpu.get_barrier_semaphore()

    def greet_col(s, _):
        pl.semaphore_signal(barrier, inc=1, device_id=(row_at, lax.rem(col_at + s, cols)), device_id_type=MESH)
        return 0

    def greet_row(s, _):
        pl.semaphore_signal(barrier, inc=1, device_id=(lax.rem(row_at + s, rows), col_at), device_id_type=MESH)
        return 0

    lax.fori_loop(1, cols, greet_col, 0)
    lax.fori_loop(1, rows, greet_row, 0)

    sh = Shifts()
    cells = [(x, y, z) for x in range(NX) for y in range(3) for z in range(3)]

    def at(x, y, z):
        return x * PLANE + y * 3 + z

    perm[...] = permutation()
    for copy in inputs:
        copy.wait()
    phases = phases_ref[...].reshape(ROWS, YZ)
    conduct = jnp.zeros((ROWS, YZ), F32)
    for phase_id in range(PHASES):
        conduct = jnp.where(phases == phase_id, cond_ref[phase_id], conduct)
    conduct = conduct * grain_ref[...].reshape(ROWS, YZ)
    parts = jnp.concatenate(pieces(conduct, 3), axis=0)
    moved = jnp.dot(parts, perm[...], preferred_element_type=F32)
    moved = (moved[2 * ROWS :] + moved[ROWS : 2 * ROWS]) + moved[:ROWS]
    for j in range(4):
        stage[j, 0:ROWS, :] = moved[:, 128 * j : 128 * j + 128]
    stage[4, 0:ROWS, 0:64] = moved[:, 512:576]

    for x in range(NX):
        for j in range(5):
            low = stage[j, pl.ds(x, 8, stride=VOX), :]
            high = stage[j, pl.ds(x + NX, 8, stride=VOX), :]
            image[x * PLANE + 2 * j] = jnp.where(sh.low, low, roll(high, 64))
            if j < 4:
                image[x * PLANE + 2 * j + 1] = jnp.where(sh.low, roll(low, 64), high)

    for x in range(NX):
        for z in range(3):
            halo[x * 3 + z] = sh.y_up(image[at(x, 0, z)])
    for x in range(NX):
        for y in range(3):
            halo[36 + x * 3 + y] = sh.z_up(image[at(x, y, 0)])
    for k in range(PLANE):
        halo[144 + k] = sh.x_swap(image[k])
    for x, y, z in cells:
        t = at(x, y, z)
        here = image[t]
        ahead = image[t + PLANE] if x < NX - 1 else halo[144 + y * 3 + z]
        face[t] = (here + ahead) * 0.5
        ahead = image[t + 3] if y < 2 else halo[x * 3 + z]
        face[CELLS + t] = (here + ahead) * 0.5
        ahead = image[t + 1] if z < 2 else halo[36 + x * 3 + y]
        face[2 * CELLS + t] = (here + ahead) * 0.5
    for x in range(NX):
        for z in range(3):
            low_face[x * 3 + z] = sh.y_down(face[CELLS + at(x, 2, z)])
    for x in range(NX):
        for y in range(3):
            low_face[36 + x * 3 + y] = sh.z_down(face[2 * CELLS + at(x, y, 2)])
    for k in range(PLANE):
        low_face[72 + k] = sh.x_swap(face[at(NX - 1, 0, 0) + k])

    zero = jnp.zeros((8, 128), F32)
    norms = [zero] * 3
    means = [zero] * 3
    for x, y, z in cells:
        t = at(x, y, z)
        back = [
            face[t - PLANE] if x > 0 else low_face[72 + y * 3 + z],
            face[CELLS + t - 3] if y > 0 else low_face[x * 3 + z],
            face[2 * CELLS + t - 1] if z > 0 else low_face[36 + x * 3 + y],
        ]
        for c in range(3):
            here = face[c * CELLS + t]
            value = here - back[c]
            rhs[c * CELLS + t] = value
            remain[c * CELLS + t] = value
            direct[c * CELLS + t] = zero
            fluct[c * CELLS + t] = zero
            norms[c] = norms[c] + value * value
            means[c] = means[c] + here

    sub = lax.broadcasted_iota(jnp.int32, (8, 128), 0)
    counts = jnp.zeros((8, 128), jnp.int32)
    for k in range(EZ):
        counts = jnp.where(sub == k, counts_ref[k], counts)

    def update(c, alpha, beta):
        base, edge = c * CELLS, c * HALO
        for first in range(0, NX, CHUNK):
            span = range(first, first + CHUNK)
            plane = {}
            for x in span:
                for k in range(PLANE):
                    t = base + x * PLANE + k
                    old = direct[t]
                    fluct[t] = fluct[t] + alpha * old
                    plane[x, k] = remain[t] + beta * old
                    direct[t] = plane[x, k]
                yield
            for x in span:
                for z in range(3):
                    halo[edge + x * 3 + z] = sh.y_up(plane[x, z])
            for x in span:
                for z in range(3):
                    halo[edge + 72 + x * 3 + z] = sh.y_down(plane[x, 6 + z])
            for x in span:
                for y in range(3):
                    halo[edge + 36 + x * 3 + y] = sh.z_up(plane[x, 3 * y])
            for x in span:
                for y in range(3):
                    halo[edge + 108 + x * 3 + y] = sh.z_down(plane[x, 3 * y + 2])
            if first == 0:
                for k in range(PLANE):
                    halo[edge + 144 + k] = sh.x_swap(plane[0, k])
            if first + CHUNK == NX:
                for k in range(PLANE):
                    halo[edge + 153 + k] = sh.x_swap(plane[NX - 1, k])

    def stencil(c, box):
        base, edge = c * CELLS, c * HALO
        acc = zero
        here = [direct[base + k] for k in range(PLANE)]
        before = [low_face[72 + k] * (halo[edge + 153 + k] - here[k]) for k in range(PLANE)]
        for x in range(NX):
            if x < NX - 1:
                ahead = [direct[base + (x + 1) * PLANE + k] for k in range(PLANE)]
            else:
                ahead = [halo[edge + 144 + k] for k in range(PLANE)]
            for y in range(3):
                if y == 0:
                    flux_y = [low_face[x * 3 + z] * (halo[edge + 72 + x * 3 + z] - here[z]) for z in range(3)]
                flux_z = low_face[36 + x * 3 + y] * (halo[edge + 108 + x * 3 + y] - here[3 * y])
                for z in range(3):
                    k = 3 * y + z
                    t = x * PLANE + k
                    v = here[k]
                    next_x = face[t] * (v - ahead[k])
                    up = here[k + 3] if y < 2 else halo[edge + x * 3 + z]
                    next_y = face[CELLS + t] * (v - up)
                    up = here[k + 1] if z < 2 else halo[edge + 36 + x * 3 + y]
                    next_z = face[2 * CELLS + t] * (v - up)
                    out = (next_x - before[k]) + ((next_y - flux_y[z]) + (next_z - flux_z))
                    image[base + t] = out
                    acc = acc + v * out
                    before[k], flux_y[z], flux_z = next_x, next_y, next_z
            here = ahead
            yield
        box.append(acc)

    def descend(c, alpha, box):
        acc = zero
        for x in range(NX):
            for t in range(c * CELLS + x * PLANE, c * CELLS + (x + 1) * PLANE):
                value = remain[t] - alpha * image[t]
                remain[t] = value
                acc = acc + value * value
            yield
        box.append(acc)

    def together(*parts):
        parts = list(parts)
        while parts:
            for part in list(parts):
                if next(part, part) is part:
                    parts.remove(part)

    def sweep(index, carry):
        norm, alpha, beta, last = carry
        live = index < counts
        box = []
        together(update(1, alpha[1], beta[1]), stencil(0, box))
        step_0 = jnp.where(live, norm[0] / total(box[0]), 0.0)
        norm_2 = total(last)
        together(update(2, alpha[2], norm_2 / norm[2]), stencil(1, box))
        step_1 = jnp.where(live, norm[1] / total(box[1]), 0.0)
        together(stencil(2, box), descend(0, step_0, box))
        acc_2, acc_0 = (box[2], box[3])
        step_2 = jnp.where(live, norm_2 / total(acc_2), 0.0)
        norm_0 = total(acc_0)
        together(descend(1, step_1, box))
        norm_1 = total(box[4])
        together(descend(2, step_2, box))
        together(update(0, step_0, norm_0 / norm[0]))
        return (norm_0, norm_1, norm_2), (step_0, step_1, step_2), (zero, norm_1 / norm[1]), box[5]

    norm = tuple(total(v) for v in norms)
    together(update(0, zero, zero))
    first = (norm, (zero,) * 3, (zero, zero), jnp.where(lane_iota() == 0, norm[2], 0.0))
    norm, alpha, beta, last = lax.fori_loop(0, MICRO_MAX - 1, sweep, first)

    box = []
    together(update(1, alpha[1], beta[1]), stencil(0, box))
    norm_2 = total(last)
    together(update(2, alpha[2], norm_2 / norm[2]), stencil(1, box))
    together(stencil(2, box))
    alpha = [
        jnp.where(counts == MICRO_MAX, top / total(low), 0.0) for top, low in zip((norm[0], norm[1], norm_2), box)
    ]

    inner = [[zero] * 3 for _ in range(3)]
    for t in range(CELLS):
        for c in range(3):
            value = fluct[c * CELLS + t] + alpha[c] * direct[c * CELLS + t]
            fluct[c * CELLS + t] = value
            for d in range(3):
                inner[d][c] = inner[d][c] + value * rhs[d * CELLS + t]
    scale = 1.0 / (VOX * YZ)
    tangent = [
        [(total(means[d] - inner[d][c]) if d == c else -total(inner[d][c])) * scale for c in range(3)]
        for d in range(3)
    ]
    lane = lane_iota()
    for d in range(3):
        for c in range(3):
            spread = jnp.sum(jnp.where(sub == (lane & 7), tangent[d][c], 0.0), axis=0, keepdims=True)
            tangent_ref[d, c] = spread[:, 0:EZ]

    slot = lane >> 3
    message = jnp.where(slot == 0, tangent[0][0], jnp.where(slot == 1, tangent[1][1], tangent[2][2]))
    message = jnp.where((sub == (lane & 7)) & (slot < 3), message, 0.0)
    message = jnp.sum(message, axis=0, keepdims=True)
    low = lax.broadcasted_iota(jnp.int32, (1, 128), 1)
    for k in range(EZ):
        message = jnp.where(low == 24 + k, current_ref[k], message)
        message = jnp.where(low == 32 + k, load_ref[k], message)
    packed[...] = message
    pl.semaphore_wait(barrier, cols + rows - 2)

    x_at, z_at = col_at // 8, lax.rem(col_at, 8)
    y_at, core_at = row_at // 2, lax.rem(row_at, 2)

    def hops(steps, lengths):
        return sum(min(step, length - step) for step, length in zip(steps, lengths))

    def along_col(s, dx, dz):
        return pltpu.make_async_remote_copy(
            src_ref=packed,
            dst_ref=inbox.at[pl.ds(col_at, 1)],
            send_sem=send_a.at[s],
            recv_sem=recv_a.at[s],
            device_id=(row_at, lax.rem(x_at + dx, 4) * 8 + lax.rem(z_at + dz, 8)),
            device_id_type=MESH,
        )

    def along_row(s, dy, dc):
        return pltpu.make_async_remote_copy(
            src_ref=grid_ref.at[row_at],
            dst_ref=grid_ref.at[row_at],
            send_sem=send_b.at[s],
            recv_sem=recv_b.at[s],
            device_id=(lax.rem(y_at + dy, 4) * 2 + lax.rem(core_at + dc, 2), col_at),
            device_id_type=MESH,
        )

    col_steps = [(dx, dz) for dx in range(4) for dz in range(8) if dx or dz]
    col_steps.sort(key=lambda steps: -hops(steps, (4, 8)))
    row_steps = [(dy, dc) for dy in range(4) for dc in range(2) if dy or dc]
    row_steps.sort(key=lambda steps: -hops(steps, (4, 2)))
    col_copies = [along_col(s, *steps) for s, steps in enumerate(col_steps)]
    row_copies = [along_row(s, *steps) for s, steps in enumerate(row_steps)]

    for copy in col_copies:
        copy.start()
    inbox[pl.ds(col_at, 1), :] = message

    for c in range(3):
        for x in range(NX):
            for j in range(5):
                first = fluct[c * CELLS + x * PLANE + 2 * j]
                second = fluct[c * CELLS + x * PLANE + 2 * j + 1] if j < 4 else zero
                stage[j, pl.ds(c * ROWS + x, 8, stride=VOX), :] = jnp.where(sh.low, first, roll(second, 64))
                stage[j, pl.ds(c * ROWS + x + NX, 8, stride=VOX), :] = jnp.where(sh.low, roll(first, 64), second)
    whole = jnp.concatenate([stage[j, 0 : 3 * ROWS, :] for j in range(4)] + [stage[4, 0 : 3 * ROWS, 0:64]], axis=1)
    parts = jnp.concatenate(pieces(whole, 2), axis=0)
    moved = lax.dot_general(parts, perm[...], (((1,), (1,)), ((), ())), preferred_element_type=F32)
    moved = moved[3 * ROWS :] + moved[: 3 * ROWS]
    for c in range(3):
        states[:, c, :, :] = moved[c * ROWS : (c + 1) * ROWS].reshape(EZ, VOX, YZ)
    out = pltpu.make_async_copy(states, states_ref, out_sem)
    out.start()
    for copy in col_copies:
        copy.wait_recv()
    grid_ref[row_at] = gathered_rows(inbox, slot, sub)
    for copy in row_copies:
        copy.start()
    for copy in col_copies:
        copy.wait_send()
    for copy in row_copies:
        copy.wait()
    out.wait()


def heavy(phases, grain, phase_cond, counts, current, load):
    smem = pl.BlockSpec(memory_space=pltpu.SMEM)
    vmem = pl.BlockSpec(memory_space=pltpu.VMEM)
    hbm = pl.BlockSpec(memory_space=pl.ANY)
    field = pltpu.VMEM((3 * CELLS, 8, 128), F32)
    return pl.pallas_call(
        heavy_kernel,
        out_shape=(
            jax.ShapeDtypeStruct((EZ, 3, VOX, YZ), F32),
            jax.ShapeDtypeStruct((3, 3, 1, EZ), F32),
            jax.ShapeDtypeStruct((8, 16, 128), F32),
        ),
        in_specs=[smem, smem, smem, smem, hbm, hbm],
        out_specs=(hbm, vmem, vmem),
        scratch_shapes=[
            pltpu.VMEM((YZ, YZ), BF16),
            pltpu.VMEM((5, 3 * ROWS, 128), F32),
            field,
            pltpu.VMEM((81, 8, 128), F32),
            field, field, field, field, field,
            pltpu.VMEM((3 * HALO, 8, 128), F32),
            pltpu.VMEM((1, 128), F32),
            pltpu.VMEM((32, 128), F32),
            pltpu.VMEM((EZ, 3, VOX, YZ), F32),
            pltpu.VMEM((EZ, VOX, YZ), jnp.int32),
            pltpu.VMEM((EZ, VOX, YZ), F32),
            pltpu.SemaphoreType.DMA((32,)),
            pltpu.SemaphoreType.DMA((32,)),
            pltpu.SemaphoreType.DMA((8,)),
            pltpu.SemaphoreType.DMA((8,)),
            pltpu.SemaphoreType.DMA,
            pltpu.SemaphoreType.DMA,
            pltpu.SemaphoreType.DMA,
        ],
        compiler_params=pltpu.CompilerParams(
            vmem_limit_bytes=62 * 1024 * 1024, collective_id=0, has_side_effects=True
        ),
        name="micro",
    )(phase_cond, counts, current, load, phases, grain)


def coarse_kernel(
    grid, states_in, tangent_in, states_ref, tangent_ref, increment_ref, residual_ref, states, in_sem, out_sem
):
    i, j = lax.axis_index("row"), lax.axis_index("col")
    inward = [pltpu.make_async_copy(states_in.at[e], states.at[e], in_sem.at[e]) for e in range(EZ)]
    outward = [pltpu.make_async_copy(states.at[e], states_ref.at[e], out_sem.at[e]) for e in range(EZ)]
    for copy in inward:
        copy.start()
    tangent_ref[...] = tangent_in[...]

    lane = lane_iota()
    slot = lane >> 3
    sub = lax.broadcasted_iota(jnp.int32, (8, 128), 0)
    fields = [[roll(grid[:, 2 * f + h, :], -8 * f) for h in range(2)] for f in range(5)]
    kx, ky, kz, current, load = fields

    def ahead_y(v):
        spun = [roll(part, -8) for part in v]
        return [jnp.where(slot == 15, spun[1], spun[0]), spun[1]]

    def back_y(v):
        spun = [roll(part, 8) for part in v]
        return [spun[0], jnp.where(slot == 0, spun[0], spun[1])]

    def ahead_z(v):
        return [roll(part, -1) for part in v]

    def back_z(v):
        return [roll(part, 1) for part in v]

    def ahead_x(v):
        return [pltpu.roll(part, 7, 0) for part in v]

    def back_x(v):
        return [pltpu.roll(part, 1, 0) for part in v]

    k_in = lane & 7
    never = lane < 0
    outside = [
        ([sub == 7] * 2, [sub == 0] * 2),
        ([never, slot == 15], [slot == 0, never]),
        ([k_in == 7] * 2, [k_in == 0] * 2),
    ]
    moves = [(ahead_x, back_x), (ahead_y, back_y), (ahead_z, back_z)]
    weights = []
    centre = [jnp.zeros((8, 128), F32)] * 2
    for (pair, masks), k in zip(zip(moves, outside), (kx, ky, kz)):
        for move, mask in zip(pair, masks):
            near = move(k)
            cond = [0.5 * (k[h] + jnp.where(mask[h], 0.0, near[h])) for h in range(2)]
            centre = [centre[h] + cond[h] for h in range(2)]
            weights.append((move, [jnp.where(mask[h], 0.0, cond[h]) for h in range(2)]))

    def apply(v):
        out = [centre[h] * v[h] for h in range(2)]
        for move, weight in weights:
            near = move(v)
            out = [out[h] - weight[h] * near[h] for h in range(2)]
        return out

    def dot(a, b):
        both = a[0] * b[0] + a[1] * b[1]
        both = jnp.sum(both, axis=0, keepdims=True)
        return jnp.broadcast_to(jnp.sum(both, axis=1, keepdims=True), (8, 128))

    image = apply(current)
    residual = [load[h] - image[h] for h in range(2)]
    increment = [jnp.zeros((8, 128), F32)] * 2
    applied = apply(residual)
    norm, curve = dot(residual, residual), dot(residual, applied)
    twice = apply(applied)
    step = norm / curve
    direction, image = residual, applied
    for iteration in range(MACRO_ITERS):
        increment = [increment[h] + step * direction[h] for h in range(2)]
        residual = [residual[h] - step * image[h] for h in range(2)]
        if iteration == 0:
            for before, after in zip(inward, outward):
                before.wait()
                after.start()
        if iteration == MACRO_ITERS - 1:
            break
        applied = [applied[h] - step * twice[h] for h in range(2)]
        fresh, curve = dot(residual, residual), dot(residual, applied)
        ahead = apply(applied)
        ratio = fresh / norm
        step = fresh / (curve - ratio * (fresh / step))
        norm = fresh
        direction = [residual[h] + ratio * direction[h] for h in range(2)]
        image = [applied[h] + ratio * image[h] for h in range(2)]
        twice = [ahead[h] + ratio * twice[h] for h in range(2)]

    place = lax.rem(j, 16)

    def own(v):
        part = jnp.where(j < 16, v[0], v[1])
        part = jnp.where((sub == i) & (slot == place), part, 0.0)
        part = jnp.broadcast_to(jnp.sum(part, axis=0, keepdims=True), (8, 128))
        spun = pltpu.roll(part, lax.rem(128 - place * 8, 128), 1)
        return spun[0:1, 0:EZ]

    increment_ref[...] = own(increment)
    residual_ref[...] = own(residual)
    for copy in outward:
        copy.wait()


def coarse(grid, states, tangent):
    vmem = pl.BlockSpec(memory_space=pltpu.VMEM)
    hbm = pl.BlockSpec(memory_space=pl.ANY)
    out = jax.ShapeDtypeStruct((1, EZ), F32)
    return pl.pallas_call(
        coarse_kernel,
        out_shape=(
            jax.ShapeDtypeStruct((EZ, 3, VOX, YZ), F32),
            jax.ShapeDtypeStruct((3, 3, 1, EZ), F32),
            out,
            out,
        ),
        in_specs=[vmem, hbm, vmem],
        out_specs=(hbm, vmem, vmem, vmem),
        scratch_shapes=[
            pltpu.VMEM((EZ, 3, VOX, YZ), F32),
            pltpu.SemaphoreType.DMA((EZ,)),
            pltpu.SemaphoreType.DMA((EZ,)),
        ],
        name="coarse",
    )(grid, states, tangent)


def shards(phases, grain, phase_cond, micro_counts, current, load):
    states, tangent, grid = heavy(
        phases.reshape(EZ, VOX, YZ), grain.reshape(EZ, VOX, YZ), phase_cond,
        micro_counts.reshape(EZ), current.reshape(EZ), load.reshape(EZ),
    )
    states, tangent, increment, residual = coarse(grid, states, tangent)
    return (
        states.reshape(1, 1, EZ, 3, VOX, YZ),
        jnp.moveaxis(tangent, 3, 0).reshape(1, 1, EZ, 3, 3),
        increment.reshape(1, 1, EZ),
        residual.reshape(1, 1, EZ),
    )


def solution(mesh):
    in_specs = (
        P("row", "col", None, None, None),
        P("row", "col", None, None, None),
        P(),
        P("row", "col", None),
        P("row", "col", None),
        P("row", "col", None),
    )
    out_specs = (
        P("row", "col", None, None, None, None),
        P("row", "col", None, None, None),
        P("row", "col", None),
        P("row", "col", None),
    )
    return jax.shard_map(shards, mesh=mesh, in_specs=in_specs, out_specs=out_specs, check_vma=False)
```

```python
import functools

import jax
import jax.numpy as jnp
from jax import lax
from jax.experimental import pallas as pl
from jax.experimental.pallas import tpu as pltpu
from jax.sharding import PartitionSpec as P

VOX = 24
YZ = 576
PHASES = 3
EZ = 8
MICRO_MAX = 12
MACRO_ITERS = 8
NX = 12
PLANE = 9
CELLS = NX * PLANE
ROWS = EZ * VOX
HALO = 162
CHUNK = 3
F32 = jnp.float32
BF16 = jnp.bfloat16
MESH = pl.DeviceIdType.MESH


def lane_iota():
    return lax.broadcasted_iota(jnp.int32, (8, 128), 1)


def roll(v, shift):
    return pltpu.roll(v, shift % 128, 1)


class Shifts:
    def __init__(self):
        lane = lane_iota()
        ys = (lane >> 3) & 7
        zs = lane & 7
        self.y_up = self.gather(jnp.where(ys == 7, lane - 56, lane + 8))
        self.y_down = self.gather(jnp.where(ys == 0, lane + 56, lane - 8))
        self.z_up = self.gather(jnp.where(zs == 7, lane - 7, lane + 1))
        self.z_down = self.gather(jnp.where(zs == 0, lane + 7, lane - 1))
        self.low = lane < 64

    def gather(self, source):
        return lambda v: jnp.take_along_axis(v, source, axis=1, mode="promise_in_bounds")

    def x_swap(self, v):
        return roll(v, 64)


def pieces(v, count):
    out = []
    for _ in range(count - 1):
        part = v.astype(BF16)
        out.append(part)
        v = v - part.astype(F32)
    out.append(v.astype(BF16))
    return out


def permutation():
    col = lax.broadcasted_iota(jnp.int32, (YZ, YZ), 1)
    row = lax.broadcasted_iota(jnp.int32, (YZ, YZ), 0)
    group = col >> 6
    y_in = (group * 11) >> 5
    z_in = group - 3 * y_in
    source = (((col >> 3) & 7) * 3 + y_in) * VOX + (col & 7) * 3 + z_in
    return jnp.where(row == source, 1.0, 0.0).astype(BF16)


def total(v):
    return jnp.broadcast_to(jnp.sum(v, axis=1, keepdims=True), (8, 128))


def gathered_rows(inbox, slot, sub):
    spans = [pltpu.roll(inbox[8 * q : 8 * q + 8, :], q % 2 * 64, 1, stride=8, stride_axis=0) for q in range(4)]
    block = [jnp.zeros((8, 128), F32)] * 2
    for f in range(5):
        for h in range(2):
            both = jnp.zeros((8, 128), F32)
            for q in (0, 1):
                both = both + jnp.where(slot == ((8 * q + sub + f) & 15), spans[2 * h + q], 0.0)
            row = 2 * f + h
            line = jnp.broadcast_to(jnp.sum(both, axis=0, keepdims=True), (8, 128))
            block[row // 8] = jnp.where(sub == row % 8, line, block[row // 8])
    return jnp.concatenate(block, axis=0)


def heavy_kernel(
    cond_ref, counts_ref, current_ref, load_ref, phases_in, grain_in,
    states_ref, tangent_ref, grid_ref,
    perm, stage, face, low_face, rhs, fluct, remain, direct, image, halo, packed, inbox, states, phases_ref, grain_ref,
    send_a, recv_a, send_b, recv_b, out_sem, phases_sem, grain_sem,
):
    inputs = [
        pltpu.make_async_copy(phases_in, phases_ref, phases_sem),
        pltpu.make_async_copy(grain_in, grain_ref, grain_sem),
    ]
    for copy in inputs:
        copy.start()
    rows, cols = 8, 32
    row_at, col_at = lax.axis_index("row"), lax.axis_index("col")
    barrier = pltpu.get_barrier_semaphore()

    def greet_col(s, _):
        pl.semaphore_signal(barrier, inc=1, device_id=(row_at, lax.rem(col_at + s, cols)), device_id_type=MESH)
        return 0

    def greet_row(s, _):
        pl.semaphore_signal(barrier, inc=1, device_id=(lax.rem(row_at + s, rows), col_at), device_id_type=MESH)
        return 0

    lax.fori_loop(1, cols, greet_col, 0)
    lax.fori_loop(1, rows, greet_row, 0)

    sh = Shifts()
    cells = [(x, y, z) for x in range(NX) for y in range(3) for z in range(3)]

    def at(x, y, z):
        return x * PLANE + y * 3 + z

    perm[...] = permutation()
    for copy in inputs:
        copy.wait()
    phases = phases_ref[...].reshape(ROWS, YZ)
    conduct = jnp.zeros((ROWS, YZ), F32)
    for phase_id in range(PHASES):
        conduct = jnp.where(phases == phase_id, cond_ref[phase_id], conduct)
    conduct = conduct * grain_ref[...].reshape(ROWS, YZ)
    parts = jnp.concatenate(pieces(conduct, 3), axis=0)
    moved = jnp.dot(parts, perm[...], preferred_element_type=F32)
    moved = (moved[2 * ROWS :] + moved[ROWS : 2 * ROWS]) + moved[:ROWS]
    for j in range(4):
        stage[j, 0:ROWS, :] = moved[:, 128 * j : 128 * j + 128]
    stage[4, 0:ROWS, 0:64] = moved[:, 512:576]

    for x in range(NX):
        for j in range(5):
            low = stage[j, pl.ds(x, 8, stride=VOX), :]
            high = stage[j, pl.ds(x + NX, 8, stride=VOX), :]
            image[x * PLANE + 2 * j] = jnp.where(sh.low, low, roll(high, 64))
            if j < 4:
                image[x * PLANE + 2 * j + 1] = jnp.where(sh.low, roll(low, 64), high)

    for x in range(NX):
        for z in range(3):
            halo[x * 3 + z] = sh.y_up(image[at(x, 0, z)])
    for x in range(NX):
        for y in range(3):
            halo[36 + x * 3 + y] = sh.z_up(image[at(x, y, 0)])
    for k in range(PLANE):
        halo[144 + k] = sh.x_swap(image[k])
    for x, y, z in cells:
        t = at(x, y, z)
        here = image[t]
        ahead = image[t + PLANE] if x < NX - 1 else halo[144 + y * 3 + z]
        face[t] = (here + ahead) * 0.5
        ahead = image[t + 3] if y < 2 else halo[x * 3 + z]
        face[CELLS + t] = (here + ahead) * 0.5
        ahead = image[t + 1] if z < 2 else halo[36 + x * 3 + y]
        face[2 * CELLS + t] = (here + ahead) * 0.5
    for x in range(NX):
        for z in range(3):
            low_face[x * 3 + z] = sh.y_down(face[CELLS + at(x, 2, z)])
    for x in range(NX):
        for y in range(3):
            low_face[36 + x * 3 + y] = sh.z_down(face[2 * CELLS + at(x, y, 2)])
    for k in range(PLANE):
        low_face[72 + k] = sh.x_swap(face[at(NX - 1, 0, 0) + k])

    zero = jnp.zeros((8, 128), F32)
    norms = [zero] * 3
    means = [zero] * 3
    for x, y, z in cells:
        t = at(x, y, z)
        back = [
            face[t - PLANE] if x > 0 else low_face[72 + y * 3 + z],
            face[CELLS + t - 3] if y > 0 else low_face[x * 3 + z],
            face[2 * CELLS + t - 1] if z > 0 else low_face[36 + x * 3 + y],
        ]
        for c in range(3):
            here = face[c * CELLS + t]
            value = here - back[c]
            rhs[c * CELLS + t] = value
            remain[c * CELLS + t] = value
            direct[c * CELLS + t] = zero
            fluct[c * CELLS + t] = zero
            norms[c] = norms[c] + value * value
            means[c] = means[c] + here

    sub = lax.broadcasted_iota(jnp.int32, (8, 128), 0)
    counts = jnp.zeros((8, 128), jnp.int32)
    for k in range(EZ):
        counts = jnp.where(sub == k, counts_ref[k], counts)

    def update(c, alpha, beta):
        base, edge = c * CELLS, c * HALO
        for first in range(0, NX, CHUNK):
            span = range(first, first + CHUNK)
            plane = {}
            for x in span:
                for k in range(PLANE):
                    t = base + x * PLANE + k
                    old = direct[t]
                    fluct[t] = fluct[t] + alpha * old
                    plane[x, k] = remain[t] + beta * old
                    direct[t] = plane[x, k]
                yield
            for x in span:
                for z in range(3):
                    halo[edge + x * 3 + z] = sh.y_up(plane[x, z])
            for x in span:
                for z in range(3):
                    halo[edge + 72 + x * 3 + z] = sh.y_down(plane[x, 6 + z])
            for x in span:
                for y in range(3):
                    halo[edge + 36 + x * 3 + y] = sh.z_up(plane[x, 3 * y])
            for x in span:
                for y in range(3):
                    halo[edge + 108 + x * 3 + y] = sh.z_down(plane[x, 3 * y + 2])
            if first == 0:
                for k in range(PLANE):
                    halo[edge + 144 + k] = sh.x_swap(plane[0, k])
            if first + CHUNK == NX:
                for k in range(PLANE):
                    halo[edge + 153 + k] = sh.x_swap(plane[NX - 1, k])

    def stencil(c, box):
        base, edge = c * CELLS, c * HALO
        acc = zero
        here = [direct[base + k] for k in range(PLANE)]
        before = [low_face[72 + k] * (halo[edge + 153 + k] - here[k]) for k in range(PLANE)]
        for x in range(NX):
            if x < NX - 1:
                ahead = [direct[base + (x + 1) * PLANE + k] for k in range(PLANE)]
            else:
                ahead = [halo[edge + 144 + k] for k in range(PLANE)]
            for y in range(3):
                if y == 0:
                    flux_y = [low_face[x * 3 + z] * (halo[edge + 72 + x * 3 + z] - here[z]) for z in range(3)]
                flux_z = low_face[36 + x * 3 + y] * (halo[edge + 108 + x * 3 + y] - here[3 * y])
                for z in range(3):
                    k = 3 * y + z
                    t = x * PLANE + k
                    v = here[k]
                    next_x = face[t] * (v - ahead[k])
                    up = here[k + 3] if y < 2 else halo[edge + x * 3 + z]
                    next_y = face[CELLS + t] * (v - up)
                    up = here[k + 1] if z < 2 else halo[edge + 36 + x * 3 + y]
                    next_z = face[2 * CELLS + t] * (v - up)
                    out = (next_x - before[k]) + ((next_y - flux_y[z]) + (next_z - flux_z))
                    image[base + t] = out
                    acc = acc + v * out
                    before[k], flux_y[z], flux_z = next_x, next_y, next_z
            here = ahead
            yield
        box.append(acc)

    def descend(c, alpha, box):
        acc = zero
        for x in range(NX):
            for t in range(c * CELLS + x * PLANE, c * CELLS + (x + 1) * PLANE):
                value = remain[t] - alpha * image[t]
                remain[t] = value
                acc = acc + value * value
            yield
        box.append(acc)

    def together(*parts):
        parts = list(parts)
        while parts:
            for part in list(parts):
                if next(part, part) is part:
                    parts.remove(part)

    def sweep(index, carry):
        norm, alpha, beta, last = carry
        live = index < counts
        box = []
        together(update(1, alpha[1], beta[1]), stencil(0, box))
        step_0 = jnp.where(live, norm[0] / total(box[0]), 0.0)
        norm_2 = total(last)
        together(update(2, alpha[2], norm_2 / norm[2]), stencil(1, box))
        step_1 = jnp.where(live, norm[1] / total(box[1]), 0.0)
        together(stencil(2, box), descend(0, step_0, box))
        acc_2, acc_0 = (box[2], box[3])
        step_2 = jnp.where(live, norm_2 / total(acc_2), 0.0)
        norm_0 = total(acc_0)
        together(descend(1, step_1, box))
        norm_1 = total(box[4])
        together(descend(2, step_2, box))
        together(update(0, step_0, norm_0 / norm[0]))
        return (norm_0, norm_1, norm_2), (step_0, step_1, step_2), (zero, norm_1 / norm[1]), box[5]

    norm = tuple(total(v) for v in norms)
    together(update(0, zero, zero))
    first = (norm, (zero,) * 3, (zero, zero), jnp.where(lane_iota() == 0, norm[2], 0.0))
    norm, alpha, beta, last = lax.fori_loop(0, MICRO_MAX - 1, sweep, first)

    box = []
    together(update(1, alpha[1], beta[1]), stencil(0, box))
    norm_2 = total(last)
    together(update(2, alpha[2], norm_2 / norm[2]), stencil(1, box))
    together(stencil(2, box))
    alpha = [
        jnp.where(counts == MICRO_MAX, top / total(low), 0.0) for top, low in zip((norm[0], norm[1], norm_2), box)
    ]

    inner = [[zero] * 3 for _ in range(3)]
    for t in range(CELLS):
        for c in range(3):
            value = fluct[c * CELLS + t] + alpha[c] * direct[c * CELLS + t]
            fluct[c * CELLS + t] = value
            inner[c][c] = inner[c][c] + value * rhs[c * CELLS + t]
    scale = 1.0 / (VOX * YZ)
    tangent = [[total(means[d] - inner[d][d]) * scale if d == c else None for c in range(3)] for d in range(3)]
    lane = lane_iota()

    slot = lane >> 3
    message = jnp.where(slot == 0, tangent[0][0], jnp.where(slot == 1, tangent[1][1], tangent[2][2]))
    message = jnp.where((sub == (lane & 7)) & (slot < 3), message, 0.0)
    message = jnp.sum(message, axis=0, keepdims=True)
    low = lax.broadcasted_iota(jnp.int32, (1, 128), 1)
    for k in range(EZ):
        message = jnp.where(low == 24 + k, current_ref[k], message)
        message = jnp.where(low == 32 + k, load_ref[k], message)
    packed[...] = message
    pl.semaphore_wait(barrier, cols + rows - 2)

    x_at, z_at = col_at // 8, lax.rem(col_at, 8)
    y_at, core_at = row_at // 2, lax.rem(row_at, 2)

    def hops(steps, lengths):
        return sum(min(step, length - step) for step, length in zip(steps, lengths))

    def along_col(s, dx, dz):
        return pltpu.make_async_remote_copy(
            src_ref=packed,
            dst_ref=inbox.at[pl.ds(col_at, 1)],
            send_sem=send_a.at[s],
            recv_sem=recv_a.at[s],
            device_id=(row_at, lax.rem(x_at + dx, 4) * 8 + lax.rem(z_at + dz, 8)),
            device_id_type=MESH,
        )

    def along_row(s, dy, dc):
        return pltpu.make_async_remote_copy(
            src_ref=grid_ref.at[row_at],
            dst_ref=grid_ref.at[row_at],
            send_sem=send_b.at[s],
            recv_sem=recv_b.at[s],
            device_id=(lax.rem(y_at + dy, 4) * 2 + lax.rem(core_at + dc, 2), col_at),
            device_id_type=MESH,
        )

    col_steps = [(dx, dz) for dx in range(4) for dz in range(8) if dx or dz]
    col_steps.sort(key=lambda steps: -hops(steps, (4, 8)))
    row_steps = [(dy, dc) for dy in range(4) for dc in range(2) if dy or dc]
    row_steps.sort(key=lambda steps: -hops(steps, (4, 2)))
    col_copies = [along_col(s, *steps) for s, steps in enumerate(col_steps)]
    row_copies = [along_row(s, *steps) for s, steps in enumerate(row_steps)]

    for copy in col_copies:
        copy.start()
    inbox[pl.ds(col_at, 1), :] = message

    for t in range(CELLS):
        for c in range(3):
            value = fluct[c * CELLS + t]
            for d in range(3):
                if d != c:
                    inner[d][c] = inner[d][c] + value * rhs[d * CELLS + t]
    for d in range(3):
        for c in range(3):
            entry = tangent[d][c] if d == c else -total(inner[d][c]) * scale
            spread = jnp.sum(jnp.where(sub == (lane & 7), entry, 0.0), axis=0, keepdims=True)
            tangent_ref[d, c] = spread[:, 0:EZ]

    for c in range(3):
        for x in range(NX):
            for j in range(5):
                first = fluct[c * CELLS + x * PLANE + 2 * j]
                second = fluct[c * CELLS + x * PLANE + 2 * j + 1] if j < 4 else zero
                stage[j, pl.ds(c * ROWS + x, 8, stride=VOX), :] = jnp.where(sh.low, first, roll(second, 64))
                stage[j, pl.ds(c * ROWS + x + NX, 8, stride=VOX), :] = jnp.where(sh.low, roll(first, 64), second)
    whole = jnp.concatenate([stage[j, 0 : 3 * ROWS, :] for j in range(4)] + [stage[4, 0 : 3 * ROWS, 0:64]], axis=1)
    parts = jnp.concatenate(pieces(whole, 2), axis=0)
    moved = lax.dot_general(parts, perm[...], (((1,), (1,)), ((), ())), preferred_element_type=F32)
    moved = moved[3 * ROWS :] + moved[: 3 * ROWS]
    for c in range(3):
        states[:, c, :, :] = moved[c * ROWS : (c + 1) * ROWS].reshape(EZ, VOX, YZ)
    out = pltpu.make_async_copy(states, states_ref, out_sem)
    out.start()
    for copy in col_copies:
        copy.wait_recv()
    grid_ref[row_at] = gathered_rows(inbox, slot, sub)
    for copy in row_copies:
        copy.start()
    for copy in col_copies:
        copy.wait_send()
    for copy in row_copies:
        copy.wait()
    out.wait()


def heavy(phases, grain, phase_cond, counts, current, load):
    smem = pl.BlockSpec(memory_space=pltpu.SMEM)
    vmem = pl.BlockSpec(memory_space=pltpu.VMEM)
    hbm = pl.BlockSpec(memory_space=pl.ANY)
    field = pltpu.VMEM((3 * CELLS, 8, 128), F32)
    return pl.pallas_call(
        heavy_kernel,
        out_shape=(
            jax.ShapeDtypeStruct((EZ, 3, VOX, YZ), F32),
            jax.ShapeDtypeStruct((3, 3, 1, EZ), F32),
            jax.ShapeDtypeStruct((8, 16, 128), F32),
        ),
        in_specs=[smem, smem, smem, smem, hbm, hbm],
        out_specs=(hbm, vmem, vmem),
        scratch_shapes=[
            pltpu.VMEM((YZ, YZ), BF16),
            pltpu.VMEM((5, 3 * ROWS, 128), F32),
            field,
            pltpu.VMEM((81, 8, 128), F32),
            field, field, field, field, field,
            pltpu.VMEM((3 * HALO, 8, 128), F32),
            pltpu.VMEM((1, 128), F32),
            pltpu.VMEM((32, 128), F32),
            pltpu.VMEM((EZ, 3, VOX, YZ), F32),
            pltpu.VMEM((EZ, VOX, YZ), jnp.int32),
            pltpu.VMEM((EZ, VOX, YZ), F32),
            pltpu.SemaphoreType.DMA((32,)),
            pltpu.SemaphoreType.DMA((32,)),
            pltpu.SemaphoreType.DMA((8,)),
            pltpu.SemaphoreType.DMA((8,)),
            pltpu.SemaphoreType.DMA,
            pltpu.SemaphoreType.DMA,
            pltpu.SemaphoreType.DMA,
        ],
        compiler_params=pltpu.CompilerParams(
            vmem_limit_bytes=62 * 1024 * 1024, collective_id=0, has_side_effects=True
        ),
        name="micro",
    )(phase_cond, counts, current, load, phases, grain)


def coarse_kernel(
    grid, states_in, tangent_in, states_ref, tangent_ref, increment_ref, residual_ref, states, in_sem, out_sem
):
    i, j = lax.axis_index("row"), lax.axis_index("col")
    inward = [pltpu.make_async_copy(states_in.at[e], states.at[e], in_sem.at[e]) for e in range(EZ)]
    outward = [pltpu.make_async_copy(states.at[e], states_ref.at[e], out_sem.at[e]) for e in range(EZ)]
    for copy in inward:
        copy.start()
    tangent_ref[...] = tangent_in[...]

    lane = lane_iota()
    slot = lane >> 3
    sub = lax.broadcasted_iota(jnp.int32, (8, 128), 0)
    fields = [[roll(grid[:, 2 * f + h, :], -8 * f) for h in range(2)] for f in range(5)]
    kx, ky, kz, current, load = fields

    def ahead_y(v):
        spun = [roll(part, -8) for part in v]
        return [jnp.where(slot == 15, spun[1], spun[0]), spun[1]]

    def back_y(v):
        spun = [roll(part, 8) for part in v]
        return [spun[0], jnp.where(slot == 0, spun[0], spun[1])]

    def ahead_z(v):
        return [roll(part, -1) for part in v]

    def back_z(v):
        return [roll(part, 1) for part in v]

    def ahead_x(v):
        return [pltpu.roll(part, 7, 0) for part in v]

    def back_x(v):
        return [pltpu.roll(part, 1, 0) for part in v]

    k_in = lane & 7
    never = lane < 0
    outside = [
        ([sub == 7] * 2, [sub == 0] * 2),
        ([never, slot == 15], [slot == 0, never]),
        ([k_in == 7] * 2, [k_in == 0] * 2),
    ]
    moves = [(ahead_x, back_x), (ahead_y, back_y), (ahead_z, back_z)]
    weights = []
    centre = [jnp.zeros((8, 128), F32)] * 2
    for (pair, masks), k in zip(zip(moves, outside), (kx, ky, kz)):
        for move, mask in zip(pair, masks):
            near = move(k)
            cond = [0.5 * (k[h] + jnp.where(mask[h], 0.0, near[h])) for h in range(2)]
            centre = [centre[h] + cond[h] for h in range(2)]
            weights.append((move, [jnp.where(mask[h], 0.0, cond[h]) for h in range(2)]))

    def apply(v):
        out = [centre[h] * v[h] for h in range(2)]
        for move, weight in weights:
            near = move(v)
            out = [out[h] - weight[h] * near[h] for h in range(2)]
        return out

    def dot(a, b):
        both = a[0] * b[0] + a[1] * b[1]
        both = jnp.sum(both, axis=0, keepdims=True)
        return jnp.broadcast_to(jnp.sum(both, axis=1, keepdims=True), (8, 128))

    image = apply(current)
    residual = [load[h] - image[h] for h in range(2)]
    increment = [jnp.zeros((8, 128), F32)] * 2
    applied = apply(residual)
    norm, curve = dot(residual, residual), dot(residual, applied)
    twice = apply(applied)
    step = norm / curve
    direction, image = residual, applied
    for iteration in range(MACRO_ITERS):
        increment = [increment[h] + step * direction[h] for h in range(2)]
        residual = [residual[h] - step * image[h] for h in range(2)]
        if iteration == 0:
            for before, after in zip(inward, outward):
                before.wait()
                after.start()
        if iteration == MACRO_ITERS - 1:
            break
        applied = [applied[h] - step * twice[h] for h in range(2)]
        fresh, curve = dot(residual, residual), dot(residual, applied)
        ahead = apply(applied)
        ratio = fresh / norm
        step = fresh / (curve - ratio * (fresh / step))
        norm = fresh
        direction = [residual[h] + ratio * direction[h] for h in range(2)]
        image = [applied[h] + ratio * image[h] for h in range(2)]
        twice = [ahead[h] + ratio * twice[h] for h in range(2)]

    place = lax.rem(j, 16)

    def own(v):
        part = jnp.where(j < 16, v[0], v[1])
        part = jnp.where((sub == i) & (slot == place), part, 0.0)
        part = jnp.broadcast_to(jnp.sum(part, axis=0, keepdims=True), (8, 128))
        spun = pltpu.roll(part, lax.rem(128 - place * 8, 128), 1)
        return spun[0:1, 0:EZ]

    increment_ref[...] = own(increment)
    residual_ref[...] = own(residual)
    for copy in outward:
        copy.wait()


def coarse(grid, states, tangent):
    vmem = pl.BlockSpec(memory_space=pltpu.VMEM)
    hbm = pl.BlockSpec(memory_space=pl.ANY)
    out = jax.ShapeDtypeStruct((1, EZ), F32)
    return pl.pallas_call(
        coarse_kernel,
        out_shape=(
            jax.ShapeDtypeStruct((EZ, 3, VOX, YZ), F32),
            jax.ShapeDtypeStruct((3, 3, 1, EZ), F32),
            out,
            out,
        ),
        in_specs=[vmem, hbm, vmem],
        out_specs=(hbm, vmem, vmem, vmem),
        scratch_shapes=[
            pltpu.VMEM((EZ, 3, VOX, YZ), F32),
            pltpu.SemaphoreType.DMA((EZ,)),
            pltpu.SemaphoreType.DMA((EZ,)),
        ],
        name="coarse",
    )(grid, states, tangent)


def shards(phases, grain, phase_cond, micro_counts, current, load):
    states, tangent, grid = heavy(
        phases.reshape(EZ, VOX, YZ), grain.reshape(EZ, VOX, YZ), phase_cond,
        micro_counts.reshape(EZ), current.reshape(EZ), load.reshape(EZ),
    )
    states, tangent, increment, residual = coarse(grid, states, tangent)
    return (
        states.reshape(1, 1, EZ, 3, VOX, YZ),
        jnp.moveaxis(tangent, 3, 0).reshape(1, 1, EZ, 3, 3),
        increment.reshape(1, 1, EZ),
        residual.reshape(1, 1, EZ),
    )


def solution(mesh):
    in_specs = (
        P("row", "col", None, None, None),
        P("row", "col", None, None, None),
        P(),
        P("row", "col", None),
        P("row", "col", None),
        P("row", "col", None),
    )
    out_specs = (
        P("row", "col", None, None, None, None),
        P("row", "col", None, None, None),
        P("row", "col", None),
        P("row", "col", None),
    )
    return jax.shard_map(shards, mesh=mesh, in_specs=in_specs, out_specs=out_specs, check_vma=False)
```
